256 devices in a mesh: tensor: 4 (over y), expert: 32 (over z, x), dp: 2 (over core).
Axes of the slice: x: 4, y: 4, z: 8, core: 2. Of those that a mesh axis runs over, the one named last changes fastest.
Arguments:
- tokens: bfloat16 [8192, 2048], P(('dp', 'expert'), 'tensor'), parts along dimension 0, may hold values from -6 to 6
- expert_ids: int32 [8192, 8], P(('dp', 'expert')), parts along dimension 0, may hold values from 0 to 127, as said below
- combine_weight: bfloat16 [8192, 8], P(('dp', 'expert')), parts along dimension 0, may hold values from 0.049804688 to 1
- gate_weight: bfloat16 [128, 768, 2048], P('expert', 'tensor'), may hold values from -0.125 to 0.125
- up_weight: bfloat16 [128, 768, 2048], P('expert', 'tensor'), may hold values from -0.125 to 0.125
- down_weight: bfloat16 [128, 768, 2048], P('expert', 'tensor'), may hold values from -0.21875 to 0.21875
Outputs:
- mixed: bfloat16 [8192, 2048], P(('dp', 'expert'), 'tensor'), parts along dimension 0
The draws below stay inside these ranges and needn't reach their ends.
There are 2 independent parts, one for each index of `dp`. The reference program is written for one: setup_inputs(seed, part) draws one part's arguments, and reference() takes and returns one part's arrays. A program takes and returns all parts, laid end to end along the dimension named above; an argument that names none is the same for every part. Nothing has to cross between parts.
Inputs may be any that keep to these rules, and one draw needn't show every extreme that they name: `expert_ids`: each row names 8 different experts; expert e sits on index e // 4 of expert. The experts of one row sit on exactly 6 different indices, at most 2 on one index. Among the rows of one index of expert (aligned blocks of 128 rows), at most 48 rows name experts on any one index, and in every draw some index receives exactly 48 rows from every block. Over all blocks at most 768 rows name any one expert, and in every draw some expert is named by exactly 768 rows.
All inputs are finite; a program needn't handle non-finite values.
Results may differ from the reference program's by a relative error of at most 0.0098.
Values may be sent and summed in bfloat16 or wider, within the bound.
A program may use at most 128 MiB of HBM per device.

```python
import math
import jax
import jax.numpy as jnp
from jax import lax

D = 2048
FF = 768
TOP = 8
EXP_DEV = 4
TOK_DEV = 128
EXPERTS = 128
TOKENS = 4096


def draw_routing(key):
    device_count = EXPERTS // EXP_DEV
    block_count = TOKENS // TOK_DEV
    spread = min(6, device_count // 2)
    capacity = min(TOK_DEV * 3 // 4, 2 * TOK_DEV * spread // device_count)
    base_share = TOP // spread
    extra_share = TOP % spread
    most_share = base_share + (1 if extra_share > 0 else 0)
    key_bias, key_noise, key_favored, key_local = jax.random.split(jax.random.fold_in(key, 913), 4)
    favored = jax.random.randint(key_favored, (), 0, device_count)
    device_index = jnp.arange(device_count, dtype=jnp.int32)
    bias = jax.random.randint(key_bias, (device_count,), 0, 48)
    bias = jnp.where(device_index == favored, 100000, bias)
    noise = jax.random.randint(key_noise, (block_count, TOK_DEV, device_count), 0, 64)
    scores = ((noise + bias[None, None, :]) * 1024 + device_index[None, None, :]).astype(jnp.int32)
    block_start = jax.random.randint(key_local, (block_count, device_count), 0, EXP_DEV).astype(jnp.int32)
    shares = jnp.array([base_share + (1 if position < extra_share else 0) for position in range(spread)], jnp.int32)
    step_index = jnp.arange(most_share, dtype=jnp.int32)

    def route_block(block_scores, start_row):

        def take_row(carry, row_scores):
            counts, used = carry
            live_scores = jnp.where(counts < capacity, row_scores, -1)
            top_values, picked = lax.top_k(live_scores, spread)
            picked = picked.astype(jnp.int32)
            cursor = used[picked] + start_row[picked]
            local = ((cursor[:, None] + step_index[None, :]) % EXP_DEV).astype(jnp.int32)
            chosen = jnp.zeros((device_count,), jnp.int32).at[picked].set(1)
            used_next = used.at[picked].add(shares)
            return ((counts + chosen, used_next), (picked, local))
        zeros = jnp.zeros((device_count,), jnp.int32)
        _, outputs = lax.scan(take_row, (zeros, zeros), block_scores)
        return outputs
    picked, local = jax.vmap(route_block)(scores, block_start)
    columns = []
    for position in range(spread):
        share = base_share + (1 if position < extra_share else 0)
        columns.append(picked[:, :, position, None] * EXP_DEV + local[:, :, position, :share])
    chosen_ids = jnp.concatenate(columns, axis=-1)
    return chosen_ids.reshape(TOKENS, TOP).astype(jnp.int32)


def draw_expert_ids(key, part):
    return draw_routing(key)


def steps_of(key, extent, pieces, smallest, high):
    factor_of = 1.0
    for dim, shards_of in pieces:
        draws = jax.random.uniform(jax.random.fold_in(jax.random.fold_in(key, 6), dim), (shards_of,), jnp.float32, smallest / len(pieces), high / len(pieces))
        factor_of = factor_of * jnp.repeat(jnp.exp(draws), extent[dim] // shards_of).reshape((-1,) + (1,) * (len(extent) - 1 - dim))
    return factor_of


def bell_draw(key, dims, scale, most, pieces=(), held_as=jnp.bfloat16):
    values = jax.random.normal(key, dims, jnp.float32) * scale
    if len(pieces) > 0:
        values = steps_of(key, dims, pieces, -0.22, 0.18) * values
    return jnp.clip(values, min=-most, max=most).astype(held_as)


def setup_inputs(seed: int = 0, part: int = 0) -> dict:
    arg_keys = jax.random.split(jax.random.key(seed), 7)
    part_keys = jax.random.split(jax.random.fold_in(arg_keys[6], part), 7)
    tokens = bell_draw(part_keys[0], (TOKENS, D), 1.0, 6.0, ((0, 32), (1, 4)))
    expert_ids = draw_expert_ids(jax.random.fold_in(jax.random.fold_in(arg_keys[6], part), 71), part)
    combine_weight = jnp.clip(jnp.exp(math.log(1.0) - 2.9996462 * jax.random.uniform(part_keys[2], (TOKENS, TOP), jnp.float32) ** steps_of(part_keys[2], (TOKENS, TOP), ((0, 32),), -0.2, 0.2)), 0.049804688, 1.0).astype(jnp.bfloat16)
    gate_weight = bell_draw(arg_keys[3], (EXPERTS, FF, D), D ** -0.5, 0.125, ((0, 32), (1, 4)))
    up_weight = bell_draw(arg_keys[4], (EXPERTS, FF, D), D ** -0.5, 0.125, ((0, 32), (1, 4)))
    down_weight = bell_draw(arg_keys[5], (EXPERTS, FF, D), FF ** -0.5, 0.21875, ((0, 32), (1, 4)))
    return {"tokens": tokens, "expert_ids": expert_ids, "combine_weight": combine_weight, "gate_weight": gate_weight, "up_weight": up_weight, "down_weight": down_weight}


tile_rows = 128


def project_rows(inputs, weight_rows):
    return lax.dot_general(inputs, weight_rows, (((1,), (1,)), ((), ())), preferred_element_type=jnp.float32)


def reference(tokens, expert_ids, combine_weight, gate_weight, up_weight, down_weight):
    token_count = tokens.shape[0]
    expert_count = gate_weight.shape[0]
    top_count = expert_ids.shape[1]
    pair_count = token_count * top_count
    flat_expert = expert_ids.reshape(-1).astype(jnp.int32)
    flat_token = (jnp.arange(pair_count, dtype=jnp.int32) // top_count).astype(jnp.int32)
    flat_weight = combine_weight.reshape(-1).astype(jnp.float32)
    counts = jnp.zeros((expert_count,), jnp.int32).at[flat_expert].add(1)
    padded = ((counts + tile_rows - 1) // tile_rows * tile_rows).astype(jnp.int32)
    starts = (jnp.cumsum(padded) - padded).astype(jnp.int32)
    plain_start = (jnp.cumsum(counts) - counts).astype(jnp.int32)
    ordering = jnp.argsort(flat_expert, stable=True).astype(jnp.int32)
    sorted_expert = flat_expert[ordering]
    placement = (starts[sorted_expert] + jnp.arange(pair_count, dtype=jnp.int32) - plain_start[sorted_expert]).astype(jnp.int32)
    tile_count = pair_count // tile_rows + expert_count + 1
    slot_token = jnp.zeros((tile_count * tile_rows,), jnp.int32).at[placement].set(flat_token[ordering])
    slot_weight = jnp.zeros((tile_count * tile_rows,), jnp.float32).at[placement].set(flat_weight[ordering])
    tile_start = (jnp.arange(tile_count, dtype=jnp.int32) * tile_rows).astype(jnp.int32)
    tile_expert = jnp.clip(jnp.sum((starts[None, :] <= tile_start[:, None]).astype(jnp.int32), axis=1) - 1, 0, expert_count - 1).astype(jnp.int32)

    def visit_tile(accumulated, tile_index):
        row_tokens = lax.dynamic_slice_in_dim(slot_token, tile_index * tile_rows, tile_rows)
        row_weights = lax.dynamic_slice_in_dim(slot_weight, tile_index * tile_rows, tile_rows)
        tile_owner = tile_expert[tile_index]
        inputs = tokens[row_tokens]
        gate_value = project_rows(inputs, gate_weight[tile_owner])
        up_value = project_rows(inputs, up_weight[tile_owner])
        hidden = (jax.nn.silu(gate_value) * up_value).astype(jnp.bfloat16)
        expert_out = jnp.dot(hidden, down_weight[tile_owner], preferred_element_type=jnp.float32)
        return accumulated.at[row_tokens].add(row_weights[:, None] * expert_out), None

    accumulated, _ = lax.scan(visit_tile, jnp.zeros((token_count, tokens.shape[1]), jnp.float32), jnp.arange(tile_count, dtype=jnp.int32))
    return accumulated.astype(jnp.bfloat16)
```

```python
import functools
import jax
import jax.numpy as jnp
from jax import lax
from jax.experimental import pallas as pl
from jax.experimental.pallas import tpu as pltpu
from jax.sharding import PartitionSpec as P

NT = 4
NX = 4
NZ = 8
TOK = 128
CAP = 48
ROWS = NX * CAP
SLICE = 512
CA = 384
CB = SLICE - CA
TW = CA + NT * CB
XW = TW + 128
HID = 768
DM = NT * SLICE
LAST = NZ - 1
BF = jnp.bfloat16
F32 = jnp.float32


def dot(a, b, dims=((1,), (0,))):
    return lax.dot_general(a, b, (dims, ((), ())), preferred_element_type=F32)


def kernel(
    tok_ref, meta_ref, gate_hbm, up_hbm, down_hbm, out_ref,
    wg, wu, wd, expand, t_buf, m_buf, sel, xs_buf, xr_buf, x_buf, x_all, hid,
    p_buf, r1_buf, r2_buf, q_buf, xb_buf, zs_buf, zb_buf, acc, bs_buf, br_buf,
    w_sem, z_send, z_recv, m_send, m_recv, x_send, x_recv,
    a1_send, a1_recv, a2_send, a2_recv, r1_send, r1_recv, r2_send, r2_recv,
    xb_send, xb_recv, zb_send, zb_recv, b_send, b_recv, bb_send, bb_recv,
):
    y = lax.axis_index("tensor")
    e = lax.axis_index("expert")
    z = e // NX
    x = e % NX
    yp = (y + 1) % NT
    yo = (y + 2) % NT
    ym = (y + 3) % NT

    def at_y(j):
        return {"tensor": j}

    def at_x(j):
        return {"expert": z * NX + j}

    def at_z(j):
        return {"expert": j * NX + x}

    def rcopy(src, dst, ssem, rsem, dev):
        return pltpu.make_async_remote_copy(
            src_ref=src, dst_ref=dst, send_sem=ssem, recv_sem=rsem,
            device_id=dev, device_id_type=pl.DeviceIdType.MESH,
        )

    def rows48(j):
        return pl.ds(pl.multiple_of(j * CAP, 16), CAP)

    def bcol(j):
        return pl.ds(pl.multiple_of(CA + CB * j, 128), CB)

    def z_copies(src, slot, dev):
        return (
            rcopy(t_buf.at[src], t_buf.at[slot], z_send.at[slot], z_recv.at[slot], dev),
            rcopy(m_buf.at[src], m_buf.at[slot], m_send.at[slot], m_recv.at[slot], dev),
        )

    def x_copy(c, r):
        to = (x + r) % NX
        return rcopy(
            xs_buf.at[c, rows48(to)], xr_buf.at[c, rows48(x)],
            x_send.at[c, r - 1], x_recv.at[c, r - 1], at_x(to),
        )

    def x_arrival(c, r):
        frm = (x + NX - r) % NX
        return rcopy(
            xs_buf.at[c, rows48(frm)], xr_buf.at[c, rows48(frm)],
            x_send.at[c, r - 1], x_recv.at[c, r - 1], at_x(frm),
        )

    def a1_copy(c, k):
        return rcopy(
            xr_buf.at[c, :, pl.ds(0, CA)], x_buf.at[c, y],
            a1_send.at[c, k], a1_recv.at[c, k], at_y(ym if k else yp),
        )

    def a1_arrival(c, k):
        frm = yp if k else ym
        return rcopy(
            xr_buf.at[c, :, pl.ds(0, CA)], x_buf.at[c, frm],
            a1_send.at[c, k], a1_recv.at[c, k], at_y(frm),
        )

    half = ROWS // 2

    def a2_copy(c, k):
        blk = x_buf.at[c, yp if k else ym, pl.ds(k * half, half)]
        return rcopy(blk, blk, a2_send.at[c, k], a2_recv.at[c, k], at_y(ym if k else yp))

    def a2_arrival(c, k):
        blk = x_buf.at[c, yo, pl.ds(k * half, half)]
        return rcopy(blk, blk, a2_send.at[c, k], a2_recv.at[c, k], at_y(yp if k else ym))

    def r1_copy(c, k):
        return rcopy(
            p_buf.at[c, yo, pl.ds(k * half, half), pl.ds(0, CA)], r1_buf.at[c, k],
            r1_send.at[c, k], r1_recv.at[c, k], at_y(ym if k else yp),
        )

    def r2_copy(c, k):
        to = ym if k else yp
        return rcopy(
            p_buf.at[c, to, :, pl.ds(0, CA)], r2_buf.at[c, k],
            r2_send.at[c, k], r2_recv.at[c, k], at_y(to),
        )

    def xb_copy(c, r):
        to = (x + r) % NX
        return rcopy(
            q_buf.at[c, rows48(to)], xb_buf.at[c, rows48(x)],
            xb_send.at[c, r - 1], xb_recv.at[c, r - 1], at_x(to),
        )

    def xb_arrival(c, r):
        frm = (x + NX - r) % NX
        return rcopy(
            q_buf.at[c, rows48(frm)], xb_buf.at[c, rows48(frm)],
            xb_send.at[c, r - 1], xb_recv.at[c, r - 1], at_x(frm),
        )

    def zb_copy(c):
        dist = (c + 1) // 2
        to = jnp.where(c % 2 == 1, z + NZ - dist, z + dist) % NZ
        return rcopy(zs_buf.at[c], zb_buf.at[c], zb_send.at[c], zb_recv.at[c], at_z(to))

    def b_copy(r):
        return rcopy(
            tok_ref.at[:, pl.ds(CA, CB)], t_buf.at[0, :, bcol(y)],
            b_send.at[r - 1], b_recv.at[r - 1], at_y((y + r) % NT),
        )

    def b_arrival(r):
        frm = (y + NT - r) % NT
        return rcopy(
            tok_ref.at[:, pl.ds(CA, CB)], t_buf.at[0, :, bcol(frm)],
            b_send.at[r - 1], b_recv.at[r - 1], at_y(frm),
        )

    def bb_copy(r):
        return rcopy(
            bs_buf.at[r - 1], br_buf.at[r - 1],
            bb_send.at[r - 1], bb_recv.at[r - 1], at_y((y + r) % NT),
        )

    loads = [
        pltpu.make_async_copy(src, dst, w_sem.at[k])
        for k, (src, dst) in enumerate(((gate_hbm, wg), (up_hbm, wu), (down_hbm, wd)))
    ]
    for load in loads:
        load.start()

    barrier = pltpu.get_barrier_semaphore()
    peers = [at_y((y + r) % NT) for r in range(1, NT)]
    peers += [at_x((x + r) % NX) for r in range(1, NX)]
    peers += [at_z((z + r) % NZ) for r in range(1, NZ)]
    for peer in peers:
        pl.semaphore_signal(barrier, 1, device_id=peer, device_id_type=pl.DeviceIdType.MESH)

    t_buf[0, :, 0:CA] = tok_ref[:, 0:CA]
    t_buf[0, :, bcol(y)] = tok_ref[:, CA:SLICE]
    m_buf[0] = meta_ref[...]
    lane_q = lax.broadcasted_iota(jnp.int32, (128, HID), 0)
    hid_n = lax.broadcasted_iota(jnp.int32, (128, HID), 1)
    base = (lane_q - NX * x) * (HID // NX)
    expand[...] = jnp.where((hid_n >= base) & (hid_n < base + HID // NX), 1.0, 0.0).astype(BF)

    pl.semaphore_wait(barrier, len(peers))
    for r in (1, 3, 2):
        b_copy(r).start()
    for r in (1, 3, 2):
        b_arrival(r).wait_recv()
    for cp in z_copies(0, 1, at_z((z + 1) % NZ)):
        cp.start()

    def route(c):
        meta = m_buf[c].astype(F32)
        rel = meta[0:8] - jnp.asarray(NX * NX * z, F32)
        wts = meta[8:16]
        sub16 = lax.broadcasted_iota(jnp.int32, (16, TOK), 0)
        present = jnp.zeros((16, TOK), F32)
        rows = []
        for xx in range(NX):
            inside = (rel >= float(NX * xx)) & (rel < float(NX * xx + NX))
            row = jnp.max(jnp.where(inside, 1.0, 0.0), axis=0, keepdims=True)
            rows.append(row)
            present = jnp.where(sub16 == xx, row, present)
        t0 = lax.broadcasted_iota(jnp.int32, (TOK, TOK), 0)
        t1 = lax.broadcasted_iota(jnp.int32, (TOK, TOK), 1)
        earlier = jnp.where(t0 < t1, 1.0, 0.0).astype(BF)
        before = dot(present.astype(BF), earlier)
        slot = lax.broadcasted_iota(jnp.int32, (CAP, TOK), 0).astype(F32)
        for xx in range(NX):
            hit = (slot == before[xx : xx + 1]) & (rows[xx] > 0.5)
            sel[c, xx * CAP : (xx + 1) * CAP] = jnp.where(hit, 1.0, 0.0).astype(BF)
        sub = t0.astype(F32)
        wide = jnp.zeros((TOK, TOK), F32)
        for i in range(8):
            wide = jnp.where(sub == rel[i : i + 1], wts[i : i + 1], wide)
        s = sel[c]
        xs_buf[c, :, 0:TW] = dot(s, t_buf[c]).astype(BF)
        xs_buf[c, :, TW:XW] = dot(s, wide.astype(BF), ((1,), (1,))).astype(BF)
        xr_buf[c, rows48(x)] = xs_buf[c, rows48(x)]

    def experts(c):
        for j in range(NT):
            x_all[:, j * SLICE : j * SLICE + CA] = x_buf[c, j]
            x_all[:, j * SLICE + CA : (j + 1) * SLICE] = xr_buf[c, :, CA + CB * j : CA + CB * (j + 1)]
        rows_in = x_all[...]
        slot_w = xr_buf[c, :, TW:XW]
        for n in range(HID // 256):
            cols = slice(n * 256, (n + 1) * 256)
            gate = dot(rows_in, wg[cols], ((1,), (1,)))
            up = dot(rows_in, wu[cols], ((1,), (1,)))
            scale = dot(slot_w, expand[:, cols])
            hid[:, cols] = (gate / (1.0 + jnp.exp(-gate)) * up * scale).astype(BF)
        h = hid[...]
        for j in range(NT):
            for n in range(SLICE // 256):
                lo = j * SLICE + n * 256
                p_buf[c, j, :, n * 256 : (n + 1) * 256] = dot(h, wd[:, lo : lo + 256]).astype(BF)

    def on(c):
        return (c >= 0) & (c < NZ)

    def step(i, carry):
        c3 = i - 2

        @pl.when(on(c3))
        def _():
            for k in range(2):
                a1_arrival(c3, k).wait_recv()
                a2_copy(c3, k).start()

        c2 = i - 1

        @pl.when(on(c2))
        def _():
            for r in (1, 3, 2):
                x_arrival(c2, r).wait_recv()
            for k in range(2):
                a1_copy(c2, k).start()
            x_buf[c2, y] = xr_buf[c2, :, 0:CA]

        c5 = i - 4

        @pl.when(on(c5))
        def _():
            for k in range(2):
                to = ym if k else yp
                part = slice(k * half, (k + 1) * half)
                r1_copy(c5, k).wait_recv()
                p_buf[c5, to, part, 0:CA] = (
                    p_buf[c5, to, part, 0:CA].astype(F32) + r1_buf[c5, k].astype(F32)
                ).astype(BF)
                r2_copy(c5, k).start()

        c1 = i

        @pl.when(on(c1))
        def _():
            @pl.when(c1 > 0)
            def _():
                for cp in z_copies(0, c1, at_z(z)):
                    cp.wait_recv()

            @pl.when(c1 < NZ - 2)
            def _():
                dz = jnp.where(c1 % 2 == 1, 1, NZ - 1)
                for cp in z_copies(c1, c1 + 2, at_z((z + dz) % NZ)):
                    cp.start()

            route(c1)
            for r in (1, 3, 2):
                x_copy(c1, r).start()

        c6 = i - 5

        @pl.when(on(c6))
        def _():
            for k in range(2):
                r2_copy(c6, k).wait_recv()
            q_buf[c6, :, 0:CA] = (
                p_buf[c6, y, :, 0:CA].astype(F32)
                + r2_buf[c6, 0].astype(F32)
                + r2_buf[c6, 1].astype(F32)
            ).astype(BF)
            for j in range(NT):
                q_buf[c6, :, CA + CB * j : CA + CB * (j + 1)] = p_buf[c6, j, :, CA:SLICE]
            for r in (1, 3, 2):
                xb_copy(c6, r).start()
            xb_buf[c6, rows48(x)] = q_buf[c6, rows48(x)]

        c7 = i - 6

        @pl.when(on(c7))
        def _():
            for r in (1, 3, 2):
                xb_arrival(c7, r).wait_recv()
            share = dot(sel[c7], xb_buf[c7], ((0,), (0,)))

            @pl.when(c7 == 0)
            def _():
                acc[...] = share

            @pl.when(c7 > 0)
            def _():
                zs_buf[c7] = share.astype(BF)
                zb_copy(c7).start()

        c8 = i - 7

        @pl.when((c8 >= 1) & (c8 < NZ))
        def _():
            zb_copy(c8).wait_recv()
            acc[...] += zb_buf[c8].astype(F32)

        c4 = i - 3

        @pl.when(c4 == 0)
        def _():
            for load in loads:
                load.wait()

        @pl.when(on(c4))
        def _():
            for k in range(2):
                a2_arrival(c4, k).wait_recv()
            experts(c4)
            for k in range(2):
                r1_copy(c4, k).start()

        return carry

    lax.fori_loop(0, NZ + 7, step, 0)

    for r in (1, 3, 2):
        bs_buf[r - 1] = acc[:, bcol((y + r) % NT)].astype(BF)
        bb_copy(r).start()
    out_ref[:, 0:CA] = acc[:, 0:CA].astype(BF)
    total = acc[:, bcol(y)]
    for r in (1, 3, 2):
        bb_copy(r).wait_recv()
        total = total + br_buf[r - 1].astype(F32)
    out_ref[:, CA:SLICE] = total.astype(BF)

    def drain(c, carry):
        for k in range(2):
            a1_copy(c, k).wait_send()
            a2_copy(c, k).wait_send()
            r1_copy(c, k).wait_send()
            r2_copy(c, k).wait_send()
        for r in range(1, NX):
            x_copy(c, r).wait_send()
            xb_copy(c, r).wait_send()

        @pl.when(c > 0)
        def _():
            for cp in z_copies(0, c, at_z(z)):
                cp.wait_send()
            zb_copy(c).wait_send()

        return carry

    lax.fori_loop(0, NZ, drain, 0)
    for r in range(1, NT):
        b_copy(r).wait_send()
        bb_copy(r).wait_send()


def per_device(tokens, expert_ids, combine_weight, gate_weight, up_weight, down_weight):
    meta = jnp.concatenate([expert_ids.astype(BF), combine_weight], axis=1).T
    flat = (HID, DM)
    vmem = pl.BlockSpec(memory_space=pltpu.VMEM)
    hbm = pl.BlockSpec(memory_space=pl.ANY)
    dma = pltpu.SemaphoreType.DMA
    return pl.pallas_call(
        kernel,
        out_shape=jax.ShapeDtypeStruct((TOK, SLICE), BF),
        in_specs=[vmem, vmem, hbm, hbm, hbm],
        out_specs=vmem,
        scratch_shapes=[
            pltpu.VMEM(flat, BF), pltpu.VMEM(flat, BF), pltpu.VMEM(flat, BF),
            pltpu.VMEM((128, HID), BF),
            pltpu.VMEM((NZ, TOK, TW), BF),
            pltpu.VMEM((NZ, 16, TOK), BF),
            pltpu.VMEM((NZ, ROWS, TOK), BF),
            pltpu.VMEM((NZ, ROWS, XW), BF),
            pltpu.VMEM((NZ, ROWS, XW), BF),
            pltpu.VMEM((NZ, NT, ROWS, CA), BF),
            pltpu.VMEM((ROWS, DM), BF),
            pltpu.VMEM((ROWS, HID), BF),
            pltpu.VMEM((NZ, NT, ROWS, SLICE), BF),
            pltpu.VMEM((NZ, 2, ROWS // 2, CA), BF),
            pltpu.VMEM((NZ, 2, ROWS, CA), BF),
            pltpu.VMEM((NZ, ROWS, TW), BF),
            pltpu.VMEM((NZ, ROWS, TW), BF),
            pltpu.VMEM((NZ, TOK, TW), BF),
            pltpu.VMEM((NZ, TOK, TW), BF),
            pltpu.VMEM((TOK, TW), F32),
            pltpu.VMEM((NT - 1, TOK, CB), BF),
            pltpu.VMEM((NT - 1, TOK, CB), BF),
            dma((3,)),
            dma((NZ,)), dma((NZ,)), dma((NZ,)), dma((NZ,)),
            dma((NZ, 3)), dma((NZ, 3)),
            dma((NZ, 2)), dma((NZ, 2)), dma((NZ, 2)), dma((NZ, 2)),
            dma((NZ, 2)), dma((NZ, 2)), dma((NZ, 2)), dma((NZ, 2)),
            dma((NZ, 3)), dma((NZ, 3)),
            dma((NZ,)), dma((NZ,)),
            dma((3,)), dma((3,)), dma((3,)), dma((3,)),
        ],
        compiler_params=pltpu.CompilerParams(
            collective_id=0, has_side_effects=True, vmem_limit_bytes=60 * 2**20
        ),
        name="moe",
    )(
        tokens, meta, gate_weight.reshape(flat), up_weight.reshape(flat), down_weight.reshape(flat)
    )


def solution(mesh):
    in_specs = (
        P(("dp", "expert"), "tensor"),
        P(("dp", "expert"), None),
        P(("dp", "expert"), None),
        P("expert", "tensor", None),
        P("expert", "tensor", None),
        P("expert", "tensor", None),
    )
    out_specs = P(("dp", "expert"), "tensor")
    return jax.shard_map(
        per_device, mesh=mesh, in_specs=in_specs, out_specs=out_specs, check_vma=False
    )
```

```python
import jax
import jax.numpy as jnp
from jax import lax
from jax.experimental import pallas as pl
from jax.experimental.pallas import tpu as pltpu
from jax.sharding import PartitionSpec as P

NT = 4
NX = 4
NZ = 8
TOK = 128
CAP = 48
ROWS = NX * CAP
SLICE = 512
CA = 384
CB = SLICE - CA
TW = CA + NT * CB
XW = TW + 128
HID = 768
DM = NT * SLICE
BF = jnp.bfloat16
F32 = jnp.float32

SLOTS = 33
SCHEDULE = (
    ("select", (0, 3, 2, 6, 12, 7, 9, 10)),
    ("gather2", (6, 8, 7, 11, 16, 15, 14, 13)),
    ("gather1", (2, 6, 5, 7, 14, 10, 11, 12)),
    ("ffn", (28, 23, 14, 12, 18, 17, 16, 15)),
    ("scatter2", (31, 29, 28, 27, 24, 22, 19, 18)),
    ("merge", (-1, 32, 31, 30, 29, 26, 25, 21)),
    ("forward", (-1, 1, 0, 4, 3, 6, -1, -1)),
    ("scatter1", (30, 27, 23, 20, 19, 18, 17, 16)),
    ("unselect", (32, 31, 30, 29, 28, 25, 24, 20)),
)


def dot(a, b, dims=((1,), (0,))):
    return lax.dot_general(a, b, (dims, ((), ())), preferred_element_type=F32)


def kernel(
    tok_ref, ids_ref, comb_ref, gate_hbm, up_hbm, down_hbm, out_ref,
    wg, wu, wd, expand, t_buf, m_buf, sel, xs_buf, xr_buf, x_buf, x_all, hid,
    p_buf, r1_buf, r2_buf, q_buf, xb_buf, share_buf, zs_buf, zb_buf, acc, bs_buf, br_buf,
    w_sem, z_send, z_recv, zz_send, zz_recv, m_send, m_recv, x_send, x_recv,
    a1_send, a1_recv, a2_send, a2_recv, r1_send, r1_recv, r2_send, r2_recv,
    xb_send, xb_recv, zb_send, zb_recv, b_send, b_recv, bb_send, bb_recv,
):
    y = lax.axis_index("tensor")
    e = lax.axis_index("expert")
    z = e // NX
    x = e % NX
    yp = (y + 1) % NT
    yo = (y + 2) % NT
    ym = (y + 3) % NT

    def at_y(j):
        return {"tensor": j}

    def at_x(j):
        return {"expert": z * NX + j}

    def at_z(j):
        return {"expert": j * NX + x}

    def rcopy(src, dst, ssem, rsem, dev):
        return pltpu.make_async_remote_copy(
            src_ref=src, dst_ref=dst, send_sem=ssem, recv_sem=rsem,
            device_id=dev, device_id_type=pl.DeviceIdType.MESH,
        )

    def rows48(j):
        return pl.ds(pl.multiple_of(j * CAP, 16), CAP)

    def bcol(j):
        return pl.ds(pl.multiple_of(CA + CB * j, 128), CB)

    def z_copies(src, slot, dev):
        one, two = pl.ds(0, CA), pl.ds(CA, TW - CA)
        return (
            rcopy(m_buf.at[src], m_buf.at[slot], m_send.at[slot], m_recv.at[slot], dev),
            rcopy(t_buf.at[src, :, one], t_buf.at[slot, :, one], z_send.at[slot], z_recv.at[slot], dev),
            rcopy(t_buf.at[src, :, two], t_buf.at[slot, :, two], zz_send.at[slot], zz_recv.at[slot], dev),
        )

    def x_copy(c, r):
        to = (x + r) % NX
        return rcopy(
            xs_buf.at[c, rows48(to)], xr_buf.at[c, rows48(x)],
            x_send.at[c, r - 1], x_recv.at[c, r - 1], at_x(to),
        )

    def x_arrival(c, r):
        frm = (x + NX - r) % NX
        return rcopy(
            xs_buf.at[c, rows48(frm)], xr_buf.at[c, rows48(frm)],
            x_send.at[c, r - 1], x_recv.at[c, r - 1], at_x(frm),
        )

    def a1_copy(c, k):
        return rcopy(
            xr_buf.at[c, :, pl.ds(0, CA)], x_buf.at[c, y],
            a1_send.at[c, k], a1_recv.at[c, k], at_y(ym if k else yp),
        )

    def a1_arrival(c, k):
        frm = yp if k else ym
        return rcopy(
            xr_buf.at[c, :, pl.ds(0, CA)], x_buf.at[c, frm],
            a1_send.at[c, k], a1_recv.at[c, k], at_y(frm),
        )

    half = ROWS // 2

    def a2_copy(c, k):
        blk = x_buf.at[c, yp if k else ym, pl.ds(k * half, half)]
        return rcopy(blk, blk, a2_send.at[c, k], a2_recv.at[c, k], at_y(ym if k else yp))

    def a2_arrival(c, k):
        blk = x_buf.at[c, yo, pl.ds(k * half, half)]
        return rcopy(blk, blk, a2_send.at[c, k], a2_recv.at[c, k], at_y(yp if k else ym))

    def r1_copy(c, k):
        return rcopy(
            p_buf.at[c, yo, pl.ds(k * half, half), pl.ds(0, CA)], r1_buf.at[c, k],
            r1_send.at[c, k], r1_recv.at[c, k], at_y(ym if k else yp),
        )

    def r2_copy(c, k):
        to = ym if k else yp
        return rcopy(
            p_buf.at[c, to, :, pl.ds(0, CA)], r2_buf.at[c, k],
            r2_send.at[c, k], r2_recv.at[c, k], at_y(to),
        )

    def xb_copy(c, r):
        to = (x + r) % NX
        return rcopy(
            q_buf.at[c, rows48(to)], xb_buf.at[c, rows48(x)],
            xb_send.at[c, r - 1], xb_recv.at[c, r - 1], at_x(to),
        )

    def xb_arrival(c, r):
        frm = (x + NX - r) % NX
        return rcopy(
            q_buf.at[c, rows48(frm)], xb_buf.at[c, rows48(frm)],
            xb_send.at[c, r - 1], xb_recv.at[c, r - 1], at_x(frm),
        )

    def zb_copy(c):
        to = jnp.where(c % 2 == 1, z + NZ - 1, z + 1) % NZ
        return rcopy(zs_buf.at[c], zb_buf.at[c], zb_send.at[c], zb_recv.at[c], at_z(to))

    def b_copy(r):
        return rcopy(
            tok_ref.at[:, pl.ds(CA, CB)], t_buf.at[0, :, bcol(y)],
            b_send.at[r - 1], b_recv.at[r - 1], at_y((y + r) % NT),
        )

    def b_arrival(r):
        frm = (y + NT - r) % NT
        return rcopy(
            tok_ref.at[:, pl.ds(CA, CB)], t_buf.at[0, :, bcol(frm)],
            b_send.at[r - 1], b_recv.at[r - 1], at_y(frm),
        )

    def bb_copy(r):
        return rcopy(
            bs_buf.at[r - 1], br_buf.at[r - 1],
            bb_send.at[r - 1], bb_recv.at[r - 1], at_y((y + r) % NT),
        )

    loads = [
        pltpu.make_async_copy(src, dst, w_sem.at[k])
        for k, (src, dst) in enumerate(((gate_hbm, wg), (up_hbm, wu), (down_hbm, wd)))
    ]
    for load in loads:
        load.start()

    barrier = pltpu.get_barrier_semaphore()
    peers = [at_y((y + r) % NT) for r in range(1, NT)]
    peers += [at_x((x + r) % NX) for r in range(1, NX)]
    peers += [at_z((z + r) % NZ) for r in (1, NZ - 1)]
    for peer in peers:
        pl.semaphore_signal(barrier, 1, device_id=peer, device_id_type=pl.DeviceIdType.MESH)

    t_buf[0, :, 0:CA] = tok_ref[:, 0:CA]
    t_buf[0, :, bcol(y)] = tok_ref[:, CA:SLICE]
    d0 = lax.broadcasted_iota(jnp.int32, (TOK, TOK), 0)
    d1 = lax.broadcasted_iota(jnp.int32, (TOK, TOK), 1)
    unit = jnp.where(d0 == d1, 1.0, 0.0).astype(BF)
    ids_t = dot(ids_ref[...].astype(F32).astype(BF), unit, ((0,), (0,)))
    comb_t = dot(comb_ref[...], unit, ((0,), (0,)))
    m_buf[0] = jnp.concatenate([ids_t, comb_t], axis=0).astype(BF)
    lane_q = lax.broadcasted_iota(jnp.int32, (128, HID), 0)
    hid_n = lax.broadcasted_iota(jnp.int32, (128, HID), 1)
    base = (lane_q - NX * x) * (HID // NX)
    expand[...] = jnp.where((hid_n >= base) & (hid_n < base + HID // NX), 1.0, 0.0).astype(BF)

    pl.semaphore_wait(barrier, len(peers))
    for r in (1, 3, 2):
        b_copy(r).start()
    own = (z_copies(0, 1, at_z((z + 1) % NZ)), z_copies(0, 2, at_z((z + NZ - 1) % NZ)))
    for k in range(3):
        if k == 2:
            for r in (1, 3, 2):
                b_arrival(r).wait_recv()
        for cps in own:
            cps[k].start()

    def route(c):
        meta = m_buf[c].astype(F32)
        rel = meta[0:8] - jnp.asarray(NX * NX * z, F32)
        wts = meta[8:16]
        sub16 = lax.broadcasted_iota(jnp.int32, (16, TOK), 0)
        present = jnp.zeros((16, TOK), F32)
        rows = []
        for xx in range(NX):
            inside = (rel >= float(NX * xx)) & (rel < float(NX * xx + NX))
            row = jnp.max(jnp.where(inside, 1.0, 0.0), axis=0, keepdims=True)
            rows.append(row)
            present = jnp.where(sub16 == xx, row, present)
        t0 = lax.broadcasted_iota(jnp.int32, (TOK, TOK), 0)
        t1 = lax.broadcasted_iota(jnp.int32, (TOK, TOK), 1)
        earlier = jnp.where(t0 < t1, 1.0, 0.0).astype(BF)
        before = dot(present.astype(BF), earlier)
        slot = lax.broadcasted_iota(jnp.int32, (CAP, TOK), 0).astype(F32)
        for xx in range(NX):
            hit = (slot == before[xx : xx + 1]) & (rows[xx] > 0.5)
            sel[c, xx * CAP : (xx + 1) * CAP] = jnp.where(hit, 1.0, 0.0).astype(BF)
        sub = t0.astype(F32)
        wide = jnp.zeros((TOK, TOK), F32)
        for i in range(8):
            wide = jnp.where(sub == rel[i : i + 1], wts[i : i + 1], wide)
        s = sel[c]
        xs_buf[c, :, 0:TW] = dot(s, t_buf[c]).astype(BF)
        xs_buf[c, :, TW:XW] = dot(s, wide.astype(BF), ((1,), (1,))).astype(BF)
        xr_buf[c, rows48(x)] = xs_buf[c, rows48(x)]

    def experts(c):
        for j in range(NT):
            x_all[:, j * SLICE : j * SLICE + CA] = x_buf[c, j]
            x_all[:, j * SLICE + CA : (j + 1) * SLICE] = xr_buf[c, :, CA + CB * j : CA + CB * (j + 1)]
        rows_in = x_all[...]
        slot_w = xr_buf[c, :, TW:XW]
        for n in range(HID // 256):
            cols = slice(n * 256, (n + 1) * 256)
            gate = dot(rows_in, wg[cols], ((1,), (1,)))
            up = dot(rows_in, wu[cols], ((1,), (1,)))
            scale = dot(slot_w, expand[:, cols])
            hid[:, cols] = (gate / (1.0 + jnp.exp(-gate)) * up * scale).astype(BF)
        h = hid[...]
        for j in range(NT):
            for n in range(SLICE // 256):
                lo = j * SLICE + n * 256
                p_buf[c, j, :, n * 256 : (n + 1) * 256] = dot(h, wd[:, lo : lo + 256]).astype(BF)

    def forward(c):
        for cp in z_copies(0, c, at_z(z)):
            cp.wait_recv()
        dz = jnp.where(c % 2 == 1, 1, NZ - 1)
        for cp in z_copies(c, c + 2, at_z((z + dz) % NZ)):
            cp.start()

    def select(c):
        @pl.when(c >= NZ - 2)
        def _():
            for cp in z_copies(0, c, at_z(z)):
                cp.wait_recv()

        route(c)
        for r in (1, 3, 2):
            x_copy(c, r).start()

    def gather1(c):
        for r in (1, 3, 2):
            x_arrival(c, r).wait_recv()
        for k in range(2):
            a1_copy(c, k).start()
        x_buf[c, y] = xr_buf[c, :, 0:CA]

    def gather2(c):
        for k in range(2):
            a1_arrival(c, k).wait_recv()
            a2_copy(c, k).start()

    def ffn(c):
        for k in range(2):
            a2_arrival(c, k).wait_recv()
        experts(c)
        for k in range(2):
            r1_copy(c, k).start()

    def scatter1(c):
        for k in range(2):
            to = ym if k else yp
            part = slice(k * half, (k + 1) * half)
            r1_copy(c, k).wait_recv()
            p_buf[c, to, part, 0:CA] = (
                p_buf[c, to, part, 0:CA].astype(F32) + r1_buf[c, k].astype(F32)
            ).astype(BF)
            r2_copy(c, k).start()

    def scatter2(c):
        for k in range(2):
            r2_copy(c, k).wait_recv()
        q_buf[c, :, 0:CA] = (
            p_buf[c, y, :, 0:CA].astype(F32)
            + r2_buf[c, 0].astype(F32)
            + r2_buf[c, 1].astype(F32)
        ).astype(BF)
        for j in range(NT):
            q_buf[c, :, CA + CB * j : CA + CB * (j + 1)] = p_buf[c, j, :, CA:SLICE]
        for r in (1, 3, 2):
            xb_copy(c, r).start()
        xb_buf[c, rows48(x)] = q_buf[c, rows48(x)]

    def unselect(c):
        for r in (1, 3, 2):
            xb_arrival(c, r).wait_recv()
        share_buf[c] = dot(sel[c], xb_buf[c], ((0,), (0,)))

    def merge(c):
        @pl.when(c < NZ - 2)
        def _():
            zb_copy(c + 2).wait_recv()
            zs_buf[c] = (share_buf[c] + zb_buf[c + 2].astype(F32)).astype(BF)

        @pl.when(c >= NZ - 2)
        def _():
            zs_buf[c] = share_buf[c].astype(BF)

        zb_copy(c).start()

    stages = dict(
        forward=forward, select=select, gather1=gather1, gather2=gather2, ffn=ffn,
        scatter1=scatter1, scatter2=scatter2, unselect=unselect, merge=merge,
    )
    first_ffn = min(dict(SCHEDULE)["ffn"])

    def step(i, carry):
        @pl.when(i == first_ffn)
        def _():
            for load in loads:
                load.wait()

        for name, slots in SCHEDULE:
            chunk = jnp.int32(-1)
            for c, slot in enumerate(slots):
                if slot >= 0:
                    chunk = jnp.where(i == slot, c, chunk)

            @pl.when(chunk >= 0)
            def _(name=name, chunk=chunk):
                stages[name](chunk)

        return carry

    lax.fori_loop(0, SLOTS, step, 0)

    for c in (1, 2):
        zb_copy(c).wait_recv()
    acc[...] = share_buf[0] + zb_buf[1].astype(F32) + zb_buf[2].astype(F32)
    for r in (1, 3, 2):
        bs_buf[r - 1] = acc[:, bcol((y + r) % NT)].astype(BF)
        bb_copy(r).start()
    out_ref[:, 0:CA] = acc[:, 0:CA].astype(BF)
    total = acc[:, bcol(y)]
    for r in (1, 3, 2):
        bb_copy(r).wait_recv()
        total = total + br_buf[r - 1].astype(F32)
    out_ref[:, CA:SLICE] = total.astype(BF)

    def drain(c, carry):
        for k in range(2):
            a1_copy(c, k).wait_send()
            a2_copy(c, k).wait_send()
            r1_copy(c, k).wait_send()
            r2_copy(c, k).wait_send()
        for r in range(1, NX):
            x_copy(c, r).wait_send()
            xb_copy(c, r).wait_send()

        @pl.when(c > 0)
        def _():
            for cp in z_copies(0, c, at_z(z)):
                cp.wait_send()
            zb_copy(c).wait_send()

        return carry

    lax.fori_loop(0, NZ, drain, 0)
    for r in range(1, NT):
        b_copy(r).wait_send()
        bb_copy(r).wait_send()


def per_device(tokens, expert_ids, combine_weight, gate_weight, up_weight, down_weight):
    flat = (HID, DM)
    vmem = pl.BlockSpec(memory_space=pltpu.VMEM)
    hbm = pl.BlockSpec(memory_space=pl.ANY)
    dma = pltpu.SemaphoreType.DMA
    return pl.pallas_call(
        kernel,
        out_shape=jax.ShapeDtypeStruct((TOK, SLICE), BF),
        in_specs=[vmem, vmem, vmem, hbm, hbm, hbm],
        out_specs=vmem,
        scratch_shapes=[
            pltpu.VMEM(flat, BF), pltpu.VMEM(flat, BF), pltpu.VMEM(flat, BF),
            pltpu.VMEM((128, HID), BF),
            pltpu.VMEM((NZ, TOK, TW), BF),
            pltpu.VMEM((NZ, 16, TOK), BF),
            pltpu.VMEM((NZ, ROWS, TOK), BF),
            pltpu.VMEM((NZ, ROWS, XW), BF),
            pltpu.VMEM((NZ, ROWS, XW), BF),
            pltpu.VMEM((NZ, NT, ROWS, CA), BF),
            pltpu.VMEM((ROWS, DM), BF),
            pltpu.VMEM((ROWS, HID), BF),
            pltpu.VMEM((NZ, NT, ROWS, SLICE), BF),
            pltpu.VMEM((NZ, 2, ROWS // 2, CA), BF),
            pltpu.VMEM((NZ, 2, ROWS, CA), BF),
            pltpu.VMEM((NZ, ROWS, TW), BF),
            pltpu.VMEM((NZ, ROWS, TW), BF),
            pltpu.VMEM((NZ, TOK, TW), F32),
            pltpu.VMEM((NZ, TOK, TW), BF),
            pltpu.VMEM((NZ, TOK, TW), BF),
            pltpu.VMEM((TOK, TW), F32),
            pltpu.VMEM((NT - 1, TOK, CB), BF),
            pltpu.VMEM((NT - 1, TOK, CB), BF),
            dma((3,)),
            dma((NZ,)), dma((NZ,)), dma((NZ,)), dma((NZ,)), dma((NZ,)), dma((NZ,)),
            dma((NZ, 3)), dma((NZ, 3)),
            dma((NZ, 2)), dma((NZ, 2)), dma((NZ, 2)), dma((NZ, 2)),
            dma((NZ, 2)), dma((NZ, 2)), dma((NZ, 2)), dma((NZ, 2)),
            dma((NZ, 3)), dma((NZ, 3)),
            dma((NZ,)), dma((NZ,)),
            dma((3,)), dma((3,)), dma((3,)), dma((3,)),
        ],
        compiler_params=pltpu.CompilerParams(
            collective_id=0, has_side_effects=True, vmem_limit_bytes=60 * 2**20
        ),
        name="moe",
    )(
        tokens, expert_ids, combine_weight, gate_weight.reshape(flat), up_weight.reshape(flat), down_weight.reshape(flat)
    )


def solution(mesh):
    in_specs = (
        P(("dp", "expert"), "tensor"),
        P(("dp", "expert"), None),
        P(("dp", "expert"), None),
        P("expert", "tensor", None),
        P("expert", "tensor", None),
        P("expert", "tensor", None),
    )
    out_specs = P(("dp", "expert"), "tensor")
    return jax.shard_map(
        per_device, mesh=mesh, in_specs=in_specs, out_specs=out_specs, check_vma=False
    )
```

```python
import jax
import jax.numpy as jnp
from jax import lax
from jax.experimental import pallas as pl
from jax.experimental.pallas import tpu as pltpu
from jax.sharding import PartitionSpec as P

NT = 4
NX = 4
NZ = 8
TOK = 128
CAP = 48
ROWS = NX * CAP
HALF = ROWS // 2
SLICE = 512
AD = 256
AR = 384
BD = SLICE - AD
BR = SLICE - AR
HID = 768
DM = NT * SLICE
BF = jnp.bfloat16
F32 = jnp.float32

SLOTS = 47
SCHEDULE = (
    ("scatter2", (40, 35, 42, 34, 32, 30, 27, 29)),
    ("forward_b", (2, 7, 6, 10, 11, 16, -1, -1)),
    ("select_a", (0, 4, 3, 7, 5, 8, 11, 14)),
    ("gather2", (7, 9, 20, 14, 11, 15, 17, 19)),
    ("return_b", (35, 26, 31, 20, 25, 24, 21, 22)),
    ("merge_a", (-1, 45, 46, 42, 43, 37, 38, 31)),
    ("gather1", (5, 7, 16, 9, 8, 13, 14, 17)),
    ("unselect_b", (46, 36, 38, 22, 31, 28, 23, 27)),
    ("select_b", (2, 7, 21, 12, 11, 16, 15, 18)),
    ("merge_b", (-1, 38, 39, 33, 32, 30, 23, 27)),
    ("finish_b", (46, -1, -1, -1, -1, -1, -1, -1)),
    ("forward_a", (-1, 1, 0, 5, 3, 7, -1, -1)),
    ("scatter1", (31, 29, 35, 27, 18, 22, 21, 26)),
    ("ffn", (27, 13, 30, 17, 16, 20, 18, 21)),
    ("unselect_a", (46, 43, 44, 40, 41, 34, 36, 30)),
)


def dot(a, b, dims=((1,), (0,))):
    return lax.dot_general(a, b, (dims, ((), ())), preferred_element_type=F32)


def iota(shape, dim):
    return lax.broadcasted_iota(jnp.int32, shape, dim)


def kernel(
    tok_hbm, ids_hbm, comb_hbm, gate_hbm, up_hbm, down_hbm, out_hbm,
    wg, wu, wd, expand, ids_v, comb_v, ta, tb, meta, sel, xsa, xsb, xrb, wts, wtr, xin, x_all, hid,
    pa, pb, r1, r2, qa, xba, xbb, sha, shb, zsa, zsb, zra, zrb, bs, br, outv,
    w_sem, in_sem, out_sem, m_s, m_r, za_s, za_r, zb_s, zb_r, xa_s, xa_r, xw_s, xw_r, xb_s, xb_r,
    g1_s, g1_r, g2_s, g2_r, s1_s, s1_r, s2_s, s2_r, ya_s, ya_r, yb_s, yb_r, ca_s, ca_r, cb_s, cb_r,
    b_s, b_r, bb_s, bb_r,
):
    y = lax.axis_index("tensor")
    e = lax.axis_index("expert")
    z = e // NX
    x = e % NX
    yp = (y + 1) % NT
    yo = (y + 2) % NT
    ym = (y + 3) % NT

    def at_y(j):
        return {"tensor": j}

    def at_x(j):
        return {"expert": z * NX + j}

    def at_z(j):
        return {"expert": (j % NZ) * NX + x}

    def rcopy(src, dst, ssem, rsem, dev):
        return pltpu.make_async_remote_copy(
            src_ref=src, dst_ref=dst, send_sem=ssem, recv_sem=rsem,
            device_id=dev, device_id_type=pl.DeviceIdType.MESH,
        )

    def rows48(j):
        return pl.ds(pl.multiple_of(j * CAP, 16), CAP)

    def bcol(j, width):
        return pl.ds(pl.multiple_of(width * j, 128), width)

    def m_copy(src, slot, dev):
        return rcopy(meta.at[src], meta.at[slot], m_s.at[slot], m_r.at[slot], dev)

    def za_copy(src, slot, dev):
        return rcopy(ta.at[src], ta.at[slot], za_s.at[slot], za_r.at[slot], dev)

    def zb_copy(src, slot, dev):
        return rcopy(tb.at[src], tb.at[slot], zb_s.at[slot], zb_r.at[slot], dev)

    def xa_copy(c, r, frm, to):
        return rcopy(
            xsa.at[c, rows48(to)], xin.at[c, y, rows48(frm)],
            xa_s.at[c, r - 1], xa_r.at[c, r - 1], at_x(to),
        )

    def xw_copy(c, r, frm, to):
        return rcopy(wts.at[c, to], wtr.at[c, frm], xw_s.at[c, r - 1], xw_r.at[c, r - 1], at_x(to))

    def xb_copy(c, r, frm, to):
        return rcopy(
            xsb.at[c, rows48(to)], xrb.at[c, rows48(frm)],
            xb_s.at[c, r - 1], xb_r.at[c, r - 1], at_x(to),
        )

    def ya_copy(c, r, frm, to):
        return rcopy(
            qa.at[c, rows48(to)], xba.at[c, rows48(frm)],
            ya_s.at[c, r - 1], ya_r.at[c, r - 1], at_x(to),
        )

    def yb_copy(c, r, frm, to):
        return rcopy(
            pb.at[c, rows48(to)], xbb.at[c, rows48(frm)],
            yb_s.at[c, r - 1], yb_r.at[c, r - 1], at_x(to),
        )

    def to_x(copy, c, r):
        return copy(c, r, x, (x + r) % NX)

    def from_x(copy, c, r):
        frm = (x + NX - r) % NX
        return copy(c, r, frm, frm)

    def g1_copy(c, k):
        return rcopy(xin.at[c, y], xin.at[c, y], g1_s.at[c, k], g1_r.at[c, k], at_y(ym if k else yp))

    def g1_arrival(c, k):
        frm = yp if k else ym
        return rcopy(xin.at[c, frm], xin.at[c, frm], g1_s.at[c, k], g1_r.at[c, k], at_y(frm))

    def g2_copy(c, k):
        blk = xin.at[c, yp if k else ym, pl.ds(k * HALF, HALF)]
        return rcopy(blk, blk, g2_s.at[c, k], g2_r.at[c, k], at_y(ym if k else yp))

    def g2_arrival(c, k):
        blk = xin.at[c, yo, pl.ds(k * HALF, HALF)]
        return rcopy(blk, blk, g2_s.at[c, k], g2_r.at[c, k], at_y(yp if k else ym))

    def s1_copy(c, k):
        return rcopy(
            pa.at[c, yo, pl.ds(k * HALF, HALF)], r1.at[c, k],
            s1_s.at[c, k], s1_r.at[c, k], at_y(ym if k else yp),
        )

    def s2_copy(c, k):
        to = ym if k else yp
        return rcopy(pa.at[c, to], r2.at[c, k], s2_s.at[c, k], s2_r.at[c, k], at_y(to))

    def home(c):
        return at_z(jnp.where(c % 2 == 1, z + NZ - 1, z + 1))

    def ca_copy(c):
        return rcopy(zsa.at[c], zra.at[c], ca_s.at[c], ca_r.at[c], home(c))

    def cb_copy(c):
        return rcopy(zsb.at[c], zrb.at[c], cb_s.at[c], cb_r.at[c], home(c))

    def b_copy(r):
        blk = tb.at[0, :, bcol(y, BD)]
        return rcopy(blk, blk, b_s.at[r - 1], b_r.at[r - 1], at_y((y + r) % NT))

    def b_arrival(r):
        frm = (y + NT - r) % NT
        blk = tb.at[0, :, bcol(frm, BD)]
        return rcopy(blk, blk, b_s.at[r - 1], b_r.at[r - 1], at_y(frm))

    def bb_copy(r):
        return rcopy(bs.at[r - 1], br.at[r - 1], bb_s.at[r - 1], bb_r.at[r - 1], at_y((y + r) % NT))

    near = (1, 3, 2)

    inputs = [
        pltpu.make_async_copy(src, dst, in_sem.at[k])
        for k, (src, dst) in enumerate((
            (tok_hbm.at[:, pl.ds(AD, BD)], tb.at[0, :, bcol(y, BD)]),
            (ids_hbm, ids_v),
            (comb_hbm, comb_v),
            (tok_hbm.at[:, pl.ds(0, AD)], ta.at[0]),
        ))
    ]
    loads = [
        pltpu.make_async_copy(src, dst, w_sem.at[k])
        for k, (src, dst) in enumerate(((gate_hbm, wg), (up_hbm, wu), (down_hbm, wd)))
    ]
    for load in inputs:
        load.start()

    barrier = pltpu.get_barrier_semaphore()
    peers = [at_y((y + r) % NT) for r in range(1, NT)]
    peers += [at_x((x + r) % NX) for r in range(1, NX)]
    peers += [at_z(z + r) for r in (1, NZ - 1)]
    for peer in peers:
        pl.semaphore_signal(barrier, 1, device_id=peer, device_id_type=pl.DeviceIdType.MESH)
    for load in loads:
        load.start()

    base = (iota((16, HID), 0) - NX * x) * (HID // NX)
    hid_n = iota((16, HID), 1)
    expand[...] = jnp.where((hid_n >= base) & (hid_n < base + HID // NX), 1.0, 0.0).astype(BF)
    for load in inputs:
        load.wait()
    meta[0] = jnp.concatenate([ids_v[...].astype(F32), comb_v[...].astype(F32)], axis=0).astype(BF)

    pl.semaphore_wait(barrier, len(peers))
    for r in near:
        b_copy(r).start()
    for copy in (za_copy, m_copy):
        for slot, dz in ((1, 1), (2, NZ - 1)):
            copy(0, slot, at_z(z + dz)).start()

    def forward_a(c):
        for copy in (m_copy, za_copy):
            copy(0, c, at_z(z)).wait_recv()
        for copy in (m_copy, za_copy):
            copy(c, c + 2, at_z(z + jnp.where(c % 2 == 1, 1, NZ - 1))).start()

    def forward_b(c):
        @pl.when(c == 0)
        def _():
            for r in near:
                b_arrival(r).wait_recv()
            zb_copy(0, 1, at_z(z + 1)).start()
            zb_copy(0, 2, at_z(z + NZ - 1)).start()

        @pl.when(c > 0)
        def _():
            zb_copy(0, c, at_z(z)).wait_recv()
            zb_copy(c, c + 2, at_z(z + jnp.where(c % 2 == 1, 1, NZ - 1))).start()

    def select_a(c):
        @pl.when(c >= NZ - 2)
        def _():
            for copy in (m_copy, za_copy):
                copy(0, c, at_z(z)).wait_recv()

        info = meta[c].astype(F32)
        rel = info[0:8] - jnp.asarray(NX * NX * z, F32)
        comb = info[8:16]
        sub16 = iota((16, TOK), 0)
        present = jnp.zeros((16, TOK), F32)
        rows = []
        for xx in range(NX):
            inside = (rel >= float(NX * xx)) & (rel < float(NX * xx + NX))
            row = jnp.max(jnp.where(inside, 1.0, 0.0), axis=0, keepdims=True)
            rows.append(row)
            present = jnp.where(sub16 == xx, row, present)
        earlier = jnp.where(iota((TOK, TOK), 0) < iota((TOK, TOK), 1), 1.0, 0.0).astype(BF)
        before = dot(present.astype(BF), earlier)
        slot = iota((CAP, TOK), 0).astype(F32)
        wide = jnp.zeros((16, TOK), F32)
        for i in range(8):
            wide = jnp.where(sub16.astype(F32) == rel[i : i + 1], comb[i : i + 1], wide)
        wide = wide.astype(BF)
        for xx in range(NX):
            hit = (slot == before[xx : xx + 1]) & (rows[xx] > 0.5)
            block = jnp.where(hit, 1.0, 0.0).astype(BF)
            sel[c, xx * CAP : (xx + 1) * CAP] = block
            wts[c, xx, :, 0:CAP] = dot(wide, block, ((1,), (1,))).astype(BF)
        xsa[c] = dot(sel[c], ta[c]).astype(BF)
        xin[c, y, rows48(x)] = xsa[c, rows48(x)]
        wtr[c, x, :, 0:CAP] = wts[c, x, :, 0:CAP]
        for r in near:
            to_x(xa_copy, c, r).start()
        for r in near:
            to_x(xw_copy, c, r).start()

    def select_b(c):
        @pl.when(c >= NZ - 2)
        def _():
            zb_copy(0, c, at_z(z)).wait_recv()

        xsb[c] = dot(sel[c], tb[c]).astype(BF)
        xrb[c, rows48(x)] = xsb[c, rows48(x)]
        for r in near:
            to_x(xb_copy, c, r).start()

    def gather1(c):
        for r in near:
            from_x(xa_copy, c, r).wait_recv()
        for k in range(2):
            g1_copy(c, k).start()

    def gather2(c):
        for k in range(2):
            g1_arrival(c, k).wait_recv()
            g2_copy(c, k).start()

    def ffn(c):
        for r in near:
            from_x(xw_copy, c, r).wait_recv()
            from_x(xb_copy, c, r).wait_recv()
        for k in range(2):
            g2_arrival(c, k).wait_recv()
        for j in range(NT):
            x_all[:, j * SLICE : j * SLICE + AD] = xin[c, j]
            x_all[:, j * SLICE + AD : (j + 1) * SLICE] = xrb[c, :, BD * j : BD * (j + 1)]
        rows_in = x_all[...]
        for n in range(HID // 256):
            cols = slice(n * 256, (n + 1) * 256)
            gate = dot(rows_in, wg[cols], ((1,), (1,)))
            up = dot(rows_in, wu[cols], ((1,), (1,)))
            scale = jnp.concatenate(
                [dot(wtr[c, xx, :, 0:CAP], expand[:, cols], ((0,), (0,))) for xx in range(NX)], axis=0
            )
            hid[:, cols] = (gate / (1.0 + jnp.exp(-gate)) * up * scale).astype(BF)
        h = hid[...]
        for j in range(NT):
            for n in range(SLICE // 256):
                lo = n * 256
                part = dot(h, wd[:, j * SLICE + lo : j * SLICE + lo + 256]).astype(BF)
                split = min(max(AR - lo, 0), 256)
                if split:
                    pa[c, j, :, lo : lo + split] = part[:, :split]
                if split < 256:
                    at = BR * j + lo + split - AR
                    pb[c, :, at : at + 256 - split] = part[:, split:]
        for k in range(2):
            s1_copy(c, k).start()

    def scatter1(c):
        for k in range(2):
            to = ym if k else yp
            part = slice(k * HALF, (k + 1) * HALF)
            s1_copy(c, k).wait_recv()
            pa[c, to, part] = (pa[c, to, part].astype(F32) + r1[c, k].astype(F32)).astype(BF)
            s2_copy(c, k).start()

    def scatter2(c):
        for k in range(2):
            s2_copy(c, k).wait_recv()
        qa[c] = (pa[c, y].astype(F32) + r2[c, 0].astype(F32) + r2[c, 1].astype(F32)).astype(BF)
        for r in near:
            to_x(ya_copy, c, r).start()
        xba[c, rows48(x)] = qa[c, rows48(x)]

    def return_b(c):
        for r in near:
            to_x(yb_copy, c, r).start()
        xbb[c, rows48(x)] = pb[c, rows48(x)]

    def unselect_a(c):
        for r in near:
            from_x(ya_copy, c, r).wait_recv()
        sha[c] = dot(sel[c], xba[c], ((0,), (0,)))

    def unselect_b(c):
        for r in near:
            from_x(yb_copy, c, r).wait_recv()
        shb[c] = dot(sel[c], xbb[c], ((0,), (0,)))

    def merge(c, copy, share, out, arrived):
        @pl.when(c < NZ - 2)
        def _():
            copy(c + 2).wait_recv()
            out[c] = (share[c] + arrived[c + 2].astype(F32)).astype(BF)

        @pl.when(c >= NZ - 2)
        def _():
            out[c] = share[c].astype(BF)

        copy(c).start()

    def merge_a(c):
        merge(c, ca_copy, sha, zsa, zra)

    def merge_b(c):
        merge(c, cb_copy, shb, zsb, zrb)

    def finish_b(c):
        for k in (1, 2):
            cb_copy(k).wait_recv()
        shb[0] += zrb[1].astype(F32) + zrb[2].astype(F32)
        for r in near:
            bs[r - 1] = shb[0, :, bcol((y + r) % NT, BR)].astype(BF)
            bb_copy(r).start()

    stages = dict(
        forward_a=forward_a, forward_b=forward_b, select_a=select_a, select_b=select_b,
        gather1=gather1, gather2=gather2, ffn=ffn, scatter1=scatter1, scatter2=scatter2,
        return_b=return_b, unselect_a=unselect_a, unselect_b=unselect_b,
        merge_a=merge_a, merge_b=merge_b, finish_b=finish_b,
    )
    first_ffn = min(dict(SCHEDULE)["ffn"])

    def step(i, carry):
        @pl.when(i == first_ffn)
        def _():
            for load in loads:
                load.wait()

        for name, slots in SCHEDULE:
            chunk = jnp.int32(-1)
            for c, slot in enumerate(slots):
                if slot >= 0:
                    chunk = jnp.where(i == slot, c, chunk)

            @pl.when(chunk >= 0)
            def _(name=name, chunk=chunk):
                stages[name](chunk)

        return carry

    lax.fori_loop(0, SLOTS, step, 0)

    total = shb[0, :, bcol(y, BR)]
    for r in near:
        bb_copy(r).wait_recv()
        total = total + br[r - 1].astype(F32)
    outv[:, AR:SLICE] = total.astype(BF)
    for c in (1, 2):
        ca_copy(c).wait_recv()
    outv[:, 0:AR] = (sha[0] + zra[1].astype(F32) + zra[2].astype(F32)).astype(BF)
    result = pltpu.make_async_copy(outv, out_hbm, out_sem)
    result.start()

    def drain(c, carry):
        for k in range(2):
            for cp in (g1_copy, g2_copy, s1_copy, s2_copy):
                cp(c, k).wait_send()
        for r in near:
            for cp in (xa_copy, xw_copy, xb_copy, ya_copy, yb_copy):
                to_x(cp, c, r).wait_send()

        @pl.when(c > 0)
        def _():
            for copy in (m_copy, za_copy, zb_copy):
                copy(0, c, at_z(z)).wait_send()
            ca_copy(c).wait_send()
            cb_copy(c).wait_send()

        return carry

    lax.fori_loop(0, NZ, drain, 0)
    for r in near:
        b_copy(r).wait_send()
        bb_copy(r).wait_send()
    result.wait()


def per_device(tokens, expert_ids, combine_weight, gate_weight, up_weight, down_weight):
    flat = (HID, DM)
    hbm = pl.BlockSpec(memory_space=pl.ANY)
    dma = pltpu.SemaphoreType.DMA

    def vmem(*shape, dtype=BF):
        return pltpu.VMEM(shape, dtype)

    return pl.pallas_call(
        kernel,
        out_shape=jax.ShapeDtypeStruct((TOK, SLICE), BF),
        in_specs=[hbm] * 6,
        out_specs=hbm,
        scratch_shapes=[
            vmem(*flat), vmem(*flat), vmem(*flat),
            vmem(16, HID), vmem(8, TOK, dtype=jnp.int32), vmem(8, TOK),
            vmem(NZ, TOK, AD), vmem(NZ, TOK, NT * BD), vmem(NZ, 16, TOK), vmem(NZ, ROWS, TOK),
            vmem(NZ, ROWS, AD), vmem(NZ, ROWS, NT * BD), vmem(NZ, ROWS, NT * BD),
            vmem(NZ, NX, 16, 128), vmem(NZ, NX, 16, 128),
            vmem(NZ, NT, ROWS, AD), vmem(ROWS, DM), vmem(ROWS, HID),
            vmem(NZ, NT, ROWS, AR), vmem(NZ, ROWS, NT * BR),
            vmem(NZ, 2, HALF, AR), vmem(NZ, 2, ROWS, AR), vmem(NZ, ROWS, AR),
            vmem(NZ, ROWS, AR), vmem(NZ, ROWS, NT * BR),
            vmem(NZ, TOK, AR, dtype=F32), vmem(NZ, TOK, NT * BR, dtype=F32),
            vmem(NZ, TOK, AR), vmem(NZ, TOK, NT * BR),
            vmem(NZ, TOK, AR), vmem(NZ, TOK, NT * BR),
            vmem(NT - 1, TOK, BR), vmem(NT - 1, TOK, BR), vmem(TOK, SLICE),
            dma((3,)), dma((4,)), dma,
            *[dma((NZ,))] * 6,
            *[dma((NZ, 3))] * 6,
            *[dma((NZ, 2))] * 8,
            *[dma((NZ, 3))] * 4,
            *[dma((NZ,))] * 4,
            *[dma((3,))] * 4,
        ],
        compiler_params=pltpu.CompilerParams(
            collective_id=0, has_side_effects=True, vmem_limit_bytes=60 * 2**20
        ),
        name="moe",
    )(
        tokens, expert_ids.T, combine_weight.T,
        gate_weight.reshape(flat), up_weight.reshape(flat), down_weight.reshape(flat),
    )


def solution(mesh):
    in_specs = (
        P(("dp", "expert"), "tensor"),
        P(("dp", "expert"), None),
        P(("dp", "expert"), None),
        P("expert", "tensor", None),
        P("expert", "tensor", None),
        P("expert", "tensor", None),
    )
    out_specs = P(("dp", "expert"), "tensor")
    return jax.shard_map(
        per_device, mesh=mesh, in_specs=in_specs, out_specs=out_specs, check_vma=False
    )
```

```python
import jax
import jax.numpy as jnp
from jax import lax
from jax.experimental import pallas as pl
from jax.experimental.pallas import tpu as pltpu
from jax.sharding import PartitionSpec as P

NT = 4
NX = 4
NZ = 8
TOK = 128
CAP = 48
ROWS = NX * CAP
HALF = ROWS // 2
SLICE = 512
AD = 256
AR = 384
BD = SLICE - AD
BR = SLICE - AR
HID = 768
DM = NT * SLICE
BF = jnp.bfloat16
F32 = jnp.float32

SLOTS = 45
SCHEDULE = (
    ("scatter1", (39, 20, 31, 33, 21, 24, 27, 26)),
    ("select_a", (0, 1, 2, 6, 7, 11, 10, 15)),
    ("forward_a", (-1, 0, 1, 4, 6, 9, -1, -1)),
    ("gather2", (5, 9, 11, 15, 16, 18, 17, 20)),
    ("forward_b", (1, 7, 8, 12, 13, 18, -1, -1)),
    ("select_b", (3, 7, 11, 21, 16, 18, 19, 20)),
    ("return_b", (41, 34, 25, 30, 26, 21, 24, 23)),
    ("scatter2", (44, 23, 39, 38, 36, 32, 31, 29)),
    ("merge_a", (-1, 28, 44, 43, 42, 38, 37, 34)),
    ("unselect_b", (44, 40, 34, 35, 33, 24, 29, 27)),
    ("gather1", (2, 3, 4, 9, 11, 14, 13, 17)),
    ("merge_b", (-1, 40, 39, 35, 34, 30, 29, 27)),
    ("ffn", (11, 16, 18, 27, 19, 20, 21, 22)),
    ("finish_b", (44, -1, -1, -1, -1, -1, -1, -1)),
    ("unselect_a", (44, 27, 43, 42, 41, 37, 36, 33)),
)


def dot(a, b, dims=((1,), (0,))):
    return lax.dot_general(a, b, (dims, ((), ())), preferred_element_type=F32)


def iota(shape, dim):
    return lax.broadcasted_iota(jnp.int32, shape, dim)


def kernel(
    tok_hbm, ids_hbm, comb_hbm, gate_hbm, up_hbm, down_hbm, out_hbm,
    wg, wu, wd, expand, ids_v, comb_v, ta, tb, meta, sel, xsa, xsb, xrb, wts, wtr, xin, x_all, hid,
    pa, pb, r1, r2, qa, xba, xbb, sha, shb, zsa, zsb, zra, zrb, bs, br, outv,
    w_sem, in_sem, out_sem, m_s, m_r, za_s, za_r, zb_s, zb_r, xa_s, xa_r, xw_s, xw_r, xb_s, xb_r,
    g1_s, g1_r, g2_s, g2_r, s1_s, s1_r, s2_s, s2_r, ya_s, ya_r, yb_s, yb_r, ca_s, ca_r, cb_s, cb_r,
    b_s, b_r, bb_s, bb_r,
):
    y = lax.axis_index("tensor")
    e = lax.axis_index("expert")
    z = e // NX
    x = e % NX
    yp = (y + 1) % NT
    yo = (y + 2) % NT
    ym = (y + 3) % NT

    def at_y(j):
        return {"tensor": j}

    def at_x(j):
        return {"expert": z * NX + j}

    def at_z(j):
        return {"expert": (j % NZ) * NX + x}

    def rcopy(src, dst, ssem, rsem, dev):
        return pltpu.make_async_remote_copy(
            src_ref=src, dst_ref=dst, send_sem=ssem, recv_sem=rsem,
            device_id=dev, device_id_type=pl.DeviceIdType.MESH,
        )

    def rows48(j):
        return pl.ds(pl.multiple_of(j * CAP, 16), CAP)

    def bcol(j, width):
        return pl.ds(pl.multiple_of(width * j, 128), width)

    def m_copy(src, slot, dev):
        return rcopy(meta.at[src], meta.at[slot], m_s.at[slot], m_r.at[slot], dev)

    def za_copy(src, slot, dev):
        return rcopy(ta.at[src], ta.at[slot], za_s.at[slot], za_r.at[slot], dev)

    def zb_copy(src, slot, dev):
        return rcopy(tb.at[src], tb.at[slot], zb_s.at[slot], zb_r.at[slot], dev)

    def xa_copy(c, r, frm, to):
        return rcopy(
            xsa.at[c, rows48(to)], xin.at[c, y, rows48(frm)],
            xa_s.at[c, r - 1], xa_r.at[c, r - 1], at_x(to),
        )

    def xw_copy(c, r, frm, to):
        return rcopy(wts.at[c, to], wtr.at[c, frm], xw_s.at[c, r - 1], xw_r.at[c, r - 1], at_x(to))

    def xb_copy(c, r, frm, to):
        return rcopy(
            xsb.at[c, rows48(to)], xrb.at[c, rows48(frm)],
            xb_s.at[c, r - 1], xb_r.at[c, r - 1], at_x(to),
        )

    def ya_copy(c, r, frm, to):
        return rcopy(
            qa.at[c, rows48(to)], xba.at[c, rows48(frm)],
            ya_s.at[c, r - 1], ya_r.at[c, r - 1], at_x(to),
        )

    def yb_copy(c, r, frm, to):
        return rcopy(
            pb.at[c, rows48(to)], xbb.at[c, rows48(frm)],
            yb_s.at[c, r - 1], yb_r.at[c, r - 1], at_x(to),
        )

    def to_x(copy, c, r):
        return copy(c, r, x, (x + r) % NX)

    def from_x(copy, c, r):
        frm = (x + NX - r) % NX
        return copy(c, r, frm, frm)

    def g1_copy(c, k):
        return rcopy(xin.at[c, y], xin.at[c, y], g1_s.at[c, k], g1_r.at[c, k], at_y(ym if k else yp))

    def g1_arrival(c, k):
        frm = yp if k else ym
        return rcopy(xin.at[c, frm], xin.at[c, frm], g1_s.at[c, k], g1_r.at[c, k], at_y(frm))

    def g2_copy(c, k):
        blk = xin.at[c, yp if k else ym, pl.ds(k * HALF, HALF)]
        return rcopy(blk, blk, g2_s.at[c, k], g2_r.at[c, k], at_y(ym if k else yp))

    def g2_arrival(c, k):
        blk = xin.at[c, yo, pl.ds(k * HALF, HALF)]
        return rcopy(blk, blk, g2_s.at[c, k], g2_r.at[c, k], at_y(yp if k else ym))

    def s1_copy(c, k):
        return rcopy(
            pa.at[c, yo, pl.ds(k * HALF, HALF)], r1.at[c, k],
            s1_s.at[c, k], s1_r.at[c, k], at_y(ym if k else yp),
        )

    def s2_copy(c, k):
        to = ym if k else yp
        return rcopy(pa.at[c, to], r2.at[c, k], s2_s.at[c, k], s2_r.at[c, k], at_y(to))

    def homeward(c, hops):
        return at_z(jnp.where(c % 2 == 1, z + NZ - hops, z + hops))

    def ca_copy(c):
        hops = jnp.where((c + 1) // 2 == 2, 2, 1)
        return rcopy(zsa.at[c], zra.at[c], ca_s.at[c], ca_r.at[c], homeward(c, hops))

    def cb_copy(c):
        return rcopy(zsb.at[c], zrb.at[c], cb_s.at[c], cb_r.at[c], homeward(c, 1))

    def b_copy(r):
        blk = tb.at[0, :, bcol(y, BD)]
        return rcopy(blk, blk, b_s.at[r - 1], b_r.at[r - 1], at_y((y + r) % NT))

    def b_arrival(r):
        frm = (y + NT - r) % NT
        blk = tb.at[0, :, bcol(frm, BD)]
        return rcopy(blk, blk, b_s.at[r - 1], b_r.at[r - 1], at_y(frm))

    def bb_copy(r):
        return rcopy(bs.at[r - 1], br.at[r - 1], bb_s.at[r - 1], bb_r.at[r - 1], at_y((y + r) % NT))

    near = (1, 3, 2)

    inputs = [
        pltpu.make_async_copy(src, dst, in_sem.at[k])
        for k, (src, dst) in enumerate((
            (tok_hbm.at[:, pl.ds(AD, BD)], tb.at[0, :, bcol(y, BD)]),
            (ids_hbm, ids_v),
            (comb_hbm, comb_v),
            (tok_hbm.at[:, pl.ds(0, AD)], ta.at[0]),
        ))
    ]
    loads = [
        pltpu.make_async_copy(src, dst, w_sem.at[k])
        for k, (src, dst) in enumerate(((gate_hbm, wg), (up_hbm, wu), (down_hbm, wd)))
    ]
    for load in inputs:
        load.start()

    barrier = pltpu.get_barrier_semaphore()
    peers = [at_y((y + r) % NT) for r in range(1, NT)]
    peers += [at_x((x + r) % NX) for r in range(1, NX)]
    peers += [at_z(z + r) for r in (1, NZ - 1, 2, NZ - 2)]
    for peer in peers:
        pl.semaphore_signal(barrier, 1, device_id=peer, device_id_type=pl.DeviceIdType.MESH)
    for load in loads:
        load.start()

    base = (iota((16, HID), 0) - NX * x) * (HID // NX)
    hid_n = iota((16, HID), 1)
    expand[...] = jnp.where((hid_n >= base) & (hid_n < base + HID // NX), 1.0, 0.0).astype(BF)
    for load in inputs:
        load.wait()
    meta[0] = jnp.concatenate([ids_v[...].astype(F32), comb_v[...].astype(F32)], axis=0).astype(BF)

    pl.semaphore_wait(barrier, len(peers))
    for r in near:
        b_copy(r).start()
    for copy in (za_copy, m_copy):
        for slot, dz in ((1, 1), (2, NZ - 1)):
            copy(0, slot, at_z(z + dz)).start()

    def forward_a(c):
        for copy in (m_copy, za_copy):
            copy(0, c, at_z(z)).wait_recv()
        for copy in (m_copy, za_copy):
            copy(c, c + 2, at_z(z + jnp.where(c % 2 == 1, 1, NZ - 1))).start()

    def forward_b(c):
        @pl.when(c == 0)
        def _():
            for r in near:
                b_arrival(r).wait_recv()
            zb_copy(0, 1, at_z(z + 1)).start()
            zb_copy(0, 2, at_z(z + NZ - 1)).start()

        @pl.when(c > 0)
        def _():
            zb_copy(0, c, at_z(z)).wait_recv()
            zb_copy(c, c + 2, at_z(z + jnp.where(c % 2 == 1, 1, NZ - 1))).start()

    def select_a(c):
        @pl.when(c >= NZ - 2)
        def _():
            for copy in (m_copy, za_copy):
                copy(0, c, at_z(z)).wait_recv()

        info = meta[c].astype(F32)
        rel = info[0:8] - jnp.asarray(NX * NX * z, F32)
        comb = info[8:16]
        sub16 = iota((16, TOK), 0)
        present = jnp.zeros((16, TOK), F32)
        rows = []
        for xx in range(NX):
            inside = (rel >= float(NX * xx)) & (rel < float(NX * xx + NX))
            row = jnp.max(jnp.where(inside, 1.0, 0.0), axis=0, keepdims=True)
            rows.append(row)
            present = jnp.where(sub16 == xx, row, present)
        earlier = jnp.where(iota((TOK, TOK), 0) < iota((TOK, TOK), 1), 1.0, 0.0).astype(BF)
        before = dot(present.astype(BF), earlier)
        slot = iota((CAP, TOK), 0).astype(F32)
        wide = jnp.zeros((16, TOK), F32)
        for i in range(8):
            wide = jnp.where(sub16.astype(F32) == rel[i : i + 1], comb[i : i + 1], wide)
        wide = wide.astype(BF)
        for xx in range(NX):
            hit = (slot == before[xx : xx + 1]) & (rows[xx] > 0.5)
            block = jnp.where(hit, 1.0, 0.0).astype(BF)
            sel[c, xx * CAP : (xx + 1) * CAP] = block
            wts[c, xx, :, 0:CAP] = dot(wide, block, ((1,), (1,))).astype(BF)
        xsa[c] = dot(sel[c], ta[c]).astype(BF)
        xin[c, y, rows48(x)] = xsa[c, rows48(x)]
        wtr[c, x, :, 0:CAP] = wts[c, x, :, 0:CAP]
        for r in near:
            to_x(xa_copy, c, r).start()
        for r in near:
            to_x(xw_copy, c, r).start()

    def select_b(c):
        @pl.when(c >= NZ - 2)
        def _():
            zb_copy(0, c, at_z(z)).wait_recv()

        xsb[c] = dot(sel[c], tb[c]).astype(BF)
        xrb[c, rows48(x)] = xsb[c, rows48(x)]
        for r in near:
            to_x(xb_copy, c, r).start()

    def gather1(c):
        for r in near:
            from_x(xa_copy, c, r).wait_recv()
        for k in range(2):
            g1_copy(c, k).start()

    def gather2(c):
        for k in range(2):
            g1_arrival(c, k).wait_recv()
            g2_copy(c, k).start()

    def ffn(c):
        for r in near:
            from_x(xw_copy, c, r).wait_recv()
            from_x(xb_copy, c, r).wait_recv()
        for k in range(2):
            g2_arrival(c, k).wait_recv()
        for j in range(NT):
            x_all[:, j * SLICE : j * SLICE + AD] = xin[c, j]
            x_all[:, j * SLICE + AD : (j + 1) * SLICE] = xrb[c, :, BD * j : BD * (j + 1)]
        rows_in = x_all[...]
        for n in range(HID // 256):
            cols = slice(n * 256, (n + 1) * 256)
            gate = dot(rows_in, wg[cols], ((1,), (1,)))
            up = dot(rows_in, wu[cols], ((1,), (1,)))
            scale = jnp.concatenate(
                [dot(wtr[c, xx, :, 0:CAP], expand[:, cols], ((0,), (0,))) for xx in range(NX)], axis=0
            )
            hid[:, cols] = (gate / (1.0 + jnp.exp(-gate)) * up * scale).astype(BF)
        h = hid[...]
        for j in range(NT):
            for n in range(SLICE // 256):
                lo = n * 256
                part = dot(h, wd[:, j * SLICE + lo : j * SLICE + lo + 256]).astype(BF)
                split = min(max(AR - lo, 0), 256)
                if split:
                    pa[c, j, :, lo : lo + split] = part[:, :split]
                if split < 256:
                    at = BR * j + lo + split - AR
                    pb[c, :, at : at + 256 - split] = part[:, split:]
        for k in range(2):
            s1_copy(c, k).start()

    def scatter1(c):
        for k in range(2):
            to = ym if k else yp
            part = slice(k * HALF, (k + 1) * HALF)
            s1_copy(c, k).wait_recv()
            pa[c, to, part] = (pa[c, to, part].astype(F32) + r1[c, k].astype(F32)).astype(BF)
            s2_copy(c, k).start()

    def scatter2(c):
        for k in range(2):
            s2_copy(c, k).wait_recv()
        qa[c] = (pa[c, y].astype(F32) + r2[c, 0].astype(F32) + r2[c, 1].astype(F32)).astype(BF)
        for r in near:
            to_x(ya_copy, c, r).start()
        xba[c, rows48(x)] = qa[c, rows48(x)]

    def return_b(c):
        for r in near:
            to_x(yb_copy, c, r).start()
        xbb[c, rows48(x)] = pb[c, rows48(x)]

    def unselect_a(c):
        for r in near:
            from_x(ya_copy, c, r).wait_recv()
        sha[c] = dot(sel[c], xba[c], ((0,), (0,)))

    def unselect_b(c):
        for r in near:
            from_x(yb_copy, c, r).wait_recv()
        shb[c] = dot(sel[c], xbb[c], ((0,), (0,)))

    def merge(c, joins, copy, share, out, arrived):
        @pl.when(joins)
        def _():
            copy(c + 2).wait_recv()
            out[c] = (share[c] + arrived[c + 2].astype(F32)).astype(BF)

        @pl.when(jnp.logical_not(joins))
        def _():
            out[c] = share[c].astype(BF)

        copy(c).start()

    def merge_a(c):
        merge(c, (c >= 3) & (c < NZ - 2), ca_copy, sha, zsa, zra)

    def merge_b(c):
        merge(c, c < NZ - 2, cb_copy, shb, zsb, zrb)

    def finish_b(c):
        for k in (1, 2):
            cb_copy(k).wait_recv()
        shb[0] += zrb[1].astype(F32) + zrb[2].astype(F32)
        for r in near:
            bs[r - 1] = shb[0, :, bcol((y + r) % NT, BR)].astype(BF)
            bb_copy(r).start()

    stages = dict(
        forward_a=forward_a, forward_b=forward_b, select_a=select_a, select_b=select_b,
        gather1=gather1, gather2=gather2, ffn=ffn, scatter1=scatter1, scatter2=scatter2,
        return_b=return_b, unselect_a=unselect_a, unselect_b=unselect_b,
        merge_a=merge_a, merge_b=merge_b, finish_b=finish_b,
    )
    first_ffn = min(dict(SCHEDULE)["ffn"])

    def step(i, carry):
        @pl.when(i == first_ffn)
        def _():
            for load in loads:
                load.wait()

        for name, slots in SCHEDULE:
            chunk = jnp.int32(-1)
            for c, slot in enumerate(slots):
                if slot >= 0:
                    chunk = jnp.where(i == slot, c, chunk)

            @pl.when(chunk >= 0)
            def _(name=name, chunk=chunk):
                stages[name](chunk)

        return carry

    lax.fori_loop(0, SLOTS, step, 0)

    total = shb[0, :, bcol(y, BR)]
    for r in near:
        bb_copy(r).wait_recv()
        total = total + br[r - 1].astype(F32)
    outv[:, AR:SLICE] = total.astype(BF)
    total = sha[0]
    for c in (4, 3, 2, 1):
        ca_copy(c).wait_recv()
        total = total + zra[c].astype(F32)
    outv[:, 0:AR] = total.astype(BF)
    result = pltpu.make_async_copy(outv, out_hbm, out_sem)
    result.start()

    def drain(c, carry):
        for k in range(2):
            for cp in (g1_copy, g2_copy, s1_copy, s2_copy):
                cp(c, k).wait_send()
        for r in near:
            for cp in (xa_copy, xw_copy, xb_copy, ya_copy, yb_copy):
                to_x(cp, c, r).wait_send()

        @pl.when(c > 0)
        def _():
            for copy in (m_copy, za_copy, zb_copy):
                copy(0, c, at_z(z)).wait_send()
            ca_copy(c).wait_send()
            cb_copy(c).wait_send()

        return carry

    lax.fori_loop(0, NZ, drain, 0)
    for r in near:
        b_copy(r).wait_send()
        bb_copy(r).wait_send()
    result.wait()


def per_device(tokens, expert_ids, combine_weight, gate_weight, up_weight, down_weight):
    flat = (HID, DM)
    hbm = pl.BlockSpec(memory_space=pl.ANY)
    dma = pltpu.SemaphoreType.DMA

    def vmem(*shape, dtype=BF):
        return pltpu.VMEM(shape, dtype)

    return pl.pallas_call(
        kernel,
        out_shape=jax.ShapeDtypeStruct((TOK, SLICE), BF),
        in_specs=[hbm] * 6,
        out_specs=hbm,
        scratch_shapes=[
            vmem(*flat), vmem(*flat), vmem(*flat),
            vmem(16, HID), vmem(8, TOK, dtype=jnp.int32), vmem(8, TOK),
            vmem(NZ, TOK, AD), vmem(NZ, TOK, NT * BD), vmem(NZ, 16, TOK), vmem(NZ, ROWS, TOK),
            vmem(NZ, ROWS, AD), vmem(NZ, ROWS, NT * BD), vmem(NZ, ROWS, NT * BD),
            vmem(NZ, NX, 16, 128), vmem(NZ, NX, 16, 128),
            vmem(NZ, NT, ROWS, AD), vmem(ROWS, DM), vmem(ROWS, HID),
            vmem(NZ, NT, ROWS, AR), vmem(NZ, ROWS, NT * BR),
            vmem(NZ, 2, HALF, AR), vmem(NZ, 2, ROWS, AR), vmem(NZ, ROWS, AR),
            vmem(NZ, ROWS, AR), vmem(NZ, ROWS, NT * BR),
            vmem(NZ, TOK, AR, dtype=F32), vmem(NZ, TOK, NT * BR, dtype=F32),
            vmem(NZ, TOK, AR), vmem(NZ, TOK, NT * BR),
            vmem(NZ, TOK, AR), vmem(NZ, TOK, NT * BR),
            vmem(NT - 1, TOK, BR), vmem(NT - 1, TOK, BR), vmem(TOK, SLICE),
            dma((3,)), dma((4,)), dma,
            *[dma((NZ,))] * 6,
            *[dma((NZ, 3))] * 6,
            *[dma((NZ, 2))] * 8,
            *[dma((NZ, 3))] * 4,
            *[dma((NZ,))] * 4,
            *[dma((3,))] * 4,
        ],
        compiler_params=pltpu.CompilerParams(
            collective_id=0, has_side_effects=True, vmem_limit_bytes=60 * 2**20
        ),
        name="moe",
    )(
        tokens, expert_ids.T, combine_weight.T,
        gate_weight.reshape(flat), up_weight.reshape(flat), down_weight.reshape(flat),
    )


def solution(mesh):
    in_specs = (
        P(("dp", "expert"), "tensor"),
        P(("dp", "expert"), None),
        P(("dp", "expert"), None),
        P("expert", "tensor", None),
        P("expert", "tensor", None),
        P("expert", "tensor", None),
    )
    out_specs = P(("dp", "expert"), "tensor")
    return jax.shard_map(
        per_device, mesh=mesh, in_specs=in_specs, out_specs=out_specs, check_vma=False
    )
```

```python
import jax
import jax.numpy as jnp
from jax import lax
from jax.experimental import pallas as pl
from jax.experimental.pallas import tpu as pltpu
from jax.sharding import PartitionSpec as P

NT = 4
NX = 4
NZ = 8
TOK = 128
CAP = 48
ROWS = NX * CAP
HALF = ROWS // 2
SLICE = 512
AD = 256
AR = 384
BD = SLICE - AD
BR = SLICE - AR
HID = 768
DM = NT * SLICE
BF = jnp.bfloat16
F32 = jnp.float32

SLOTS = 45
SCHEDULE = (
    ("scatter2", (44, 24, 40, 39, 37, 33, 32, 29)),
    ("merge_a", (-1, 28, 44, 43, 42, 39, 38, 35)),
    ("select_a", (0, 1, 2, 6, 7, 11, 10, 15)),
    ("forward_a", (-1, 0, 1, 4, 6, 9, -1, -1)),
    ("scatter1", (39, 20, 31, 33, 21, 24, 27, 26)),
    ("gather2", (5, 9, 11, 15, 16, 18, 17, 20)),
    ("unselect_b", (44, 41, 35, 36, 33, 25, 29, 27)),
    ("forward_b", (1, 7, 8, 12, 13, 18, -1, -1)),
    ("finish_b", (44, -1, -1, -1, -1, -1, -1, -1)),
    ("select_b", (3, 7, 11, 21, 16, 18, 19, 20)),
    ("gather1", (2, 3, 4, 9, 11, 14, 13, 17)),
    ("merge_b", (-1, 41, 40, 36, 35, 30, 29, 27)),
    ("ffn", (11, 16, 18, 27, 19, 20, 22, 23)),
    ("return_b", (41, 34, 25, 29, 26, 21, 24, 23)),
    ("unselect_a", (44, 27, 43, 42, 41, 38, 37, 33)),
)


def dot(a, b, dims=((1,), (0,))):
    return lax.dot_general(a, b, (dims, ((), ())), preferred_element_type=F32)


def iota(shape, dim):
    return lax.broadcasted_iota(jnp.int32, shape, dim)


def kernel(
    tok_hbm, ids_hbm, comb_hbm, gate_hbm, up_hbm, down_hbm, out_hbm,
    wg, wu, wd, expand, ids_v, comb_v, ta, tb, meta, sel, xsa, xsb, xrb, wts, wtr, xin, x_all, hid,
    pa, pb, r1, r2, qa, xba, xbb, sha, shb, zsa, zsb, zra, zrb, bs, br, outv,
    w_sem, in_sem, out_sem, m_s, m_r, za_s, za_r, zb_s, zb_r, xa_s, xa_r, xw_s, xw_r, xb_s, xb_r,
    g1_s, g1_r, g2_s, g2_r, s1_s, s1_r, s2_s, s2_r, ya_s, ya_r, yb_s, yb_r, ca_s, ca_r, cb_s, cb_r,
    b_s, b_r, bb_s, bb_r,
):
    y = lax.axis_index("tensor")
    e = lax.axis_index("expert")
    z = e // NX
    x = e % NX
    yp = (y + 1) % NT
    yo = (y + 2) % NT
    ym = (y + 3) % NT

    def at_y(j):
        return {"tensor": j}

    def at_x(j):
        return {"expert": z * NX + j}

    def at_z(j):
        return {"expert": (j % NZ) * NX + x}

    def rcopy(src, dst, ssem, rsem, dev):
        return pltpu.make_async_remote_copy(
            src_ref=src, dst_ref=dst, send_sem=ssem, recv_sem=rsem,
            device_id=dev, device_id_type=pl.DeviceIdType.MESH,
        )

    def rows48(j):
        return pl.ds(pl.multiple_of(j * CAP, 16), CAP)

    def bcol(j, width):
        return pl.ds(pl.multiple_of(width * j, 128), width)

    def m_copy(src, slot, dev):
        return rcopy(meta.at[src], meta.at[slot], m_s.at[slot], m_r.at[slot], dev)

    def za_copy(src, slot, dev):
        return rcopy(ta.at[src], ta.at[slot], za_s.at[slot], za_r.at[slot], dev)

    def zb_copy(src, slot, dev):
        return rcopy(tb.at[src], tb.at[slot], zb_s.at[slot], zb_r.at[slot], dev)

    def xa_copy(c, r, frm, to):
        return rcopy(
            xsa.at[c, rows48(to)], xin.at[c, y, rows48(frm)],
            xa_s.at[c, r - 1], xa_r.at[c, r - 1], at_x(to),
        )

    def xw_copy(c, r, frm, to):
        return rcopy(wts.at[c, to], wtr.at[c, frm], xw_s.at[c, r - 1], xw_r.at[c, r - 1], at_x(to))

    def xb_copy(c, r, frm, to):
        return rcopy(
            xsb.at[c, rows48(to)], xrb.at[c, rows48(frm)],
            xb_s.at[c, r - 1], xb_r.at[c, r - 1], at_x(to),
        )

    def ya_copy(c, r, frm, to):
        return rcopy(
            qa.at[c, rows48(to)], xba.at[c, rows48(frm)],
            ya_s.at[c, r - 1], ya_r.at[c, r - 1], at_x(to),
        )

    def yb_copy(c, r, frm, to):
        return rcopy(
            pb.at[c, rows48(to)], xbb.at[c, rows48(frm)],
            yb_s.at[c, r - 1], yb_r.at[c, r - 1], at_x(to),
        )

    def to_x(copy, c, r):
        return copy(c, r, x, (x + r) % NX)

    def from_x(copy, c, r):
        frm = (x + NX - r) % NX
        return copy(c, r, frm, frm)

    def g1_copy(c, k):
        return rcopy(xin.at[c, y], xin.at[c, y], g1_s.at[c, k], g1_r.at[c, k], at_y(ym if k else yp))

    def g1_arrival(c, k):
        frm = yp if k else ym
        return rcopy(xin.at[c, frm], xin.at[c, frm], g1_s.at[c, k], g1_r.at[c, k], at_y(frm))

    def g2_copy(c, k):
        blk = xin.at[c, yp if k else ym, pl.ds(k * HALF, HALF)]
        return rcopy(blk, blk, g2_s.at[c, k], g2_r.at[c, k], at_y(ym if k else yp))

    def g2_arrival(c, k):
        blk = xin.at[c, yo, pl.ds(k * HALF, HALF)]
        return rcopy(blk, blk, g2_s.at[c, k], g2_r.at[c, k], at_y(yp if k else ym))

    def s1_copy(c, k):
        return rcopy(
            pa.at[c, yo, pl.ds(k * HALF, HALF)], r1.at[c, k],
            s1_s.at[c, k], s1_r.at[c, k], at_y(ym if k else yp),
        )

    def s2_copy(c, k):
        to = ym if k else yp
        return rcopy(pa.at[c, to], r2.at[c, k], s2_s.at[c, k], s2_r.at[c, k], at_y(to))

    def homeward(c, hops):
        return at_z(jnp.where(c % 2 == 1, z + NZ - hops, z + hops))

    def ca_copy(c):
        hops = jnp.where((c + 1) // 2 == 2, 2, 1)
        return rcopy(zsa.at[c], zra.at[c], ca_s.at[c], ca_r.at[c], homeward(c, hops))

    def cb_copy(c):
        return rcopy(zsb.at[c], zrb.at[c], cb_s.at[c], cb_r.at[c], homeward(c, 1))

    def b_copy(r):
        blk = tb.at[0, :, bcol(y, BD)]
        return rcopy(blk, blk, b_s.at[r - 1], b_r.at[r - 1], at_y((y + r) % NT))

    def b_arrival(r):
        frm = (y + NT - r) % NT
        blk = tb.at[0, :, bcol(frm, BD)]
        return rcopy(blk, blk, b_s.at[r - 1], b_r.at[r - 1], at_y(frm))

    def bb_copy(r):
        return rcopy(bs.at[r - 1], br.at[r - 1], bb_s.at[r - 1], bb_r.at[r - 1], at_y((y + r) % NT))

    near = (2, 1, 3)

    inputs = [
        pltpu.make_async_copy(src, dst, in_sem.at[k])
        for k, (src, dst) in enumerate((
            (tok_hbm.at[:, pl.ds(AD, BD)], tb.at[0, :, bcol(y, BD)]),
            (ids_hbm, ids_v),
            (comb_hbm, comb_v),
            (tok_hbm.at[:, pl.ds(0, AD)], ta.at[0]),
        ))
    ]
    loads = [
        pltpu.make_async_copy(src, dst, w_sem.at[k])
        for k, (src, dst) in enumerate(((gate_hbm, wg), (up_hbm, wu), (down_hbm, wd)))
    ]
    for load in inputs:
        load.start()

    barrier = pltpu.get_barrier_semaphore()
    peers = [at_y((y + r) % NT) for r in range(1, NT)]
    peers += [at_x((x + r) % NX) for r in range(1, NX)]
    peers += [at_z(z + r) for r in (1, NZ - 1, 2, NZ - 2)]
    for peer in peers:
        pl.semaphore_signal(barrier, 1, device_id=peer, device_id_type=pl.DeviceIdType.MESH)
    for load in loads:
        load.start()

    base = (iota((16, HID), 0) - NX * x) * (HID // NX)
    hid_n = iota((16, HID), 1)
    expand[...] = jnp.where((hid_n >= base) & (hid_n < base + HID // NX), 1.0, 0.0).astype(BF)
    for load in inputs:
        load.wait()
    meta[0] = jnp.concatenate([ids_v[...].astype(F32), comb_v[...].astype(F32)], axis=0).astype(BF)

    def selection(c):
        info = meta[c].astype(F32)
        rel = info[0:8] - jnp.asarray(NX * NX * z, F32)
        comb = info[8:16]
        sub16 = iota((16, TOK), 0)
        present = jnp.zeros((16, TOK), F32)
        rows = []
        for xx in range(NX):
            inside = (rel >= float(NX * xx)) & (rel < float(NX * xx + NX))
            row = jnp.max(jnp.where(inside, 1.0, 0.0), axis=0, keepdims=True)
            rows.append(row)
            present = jnp.where(sub16 == xx, row, present)
        earlier = jnp.where(iota((TOK, TOK), 0) < iota((TOK, TOK), 1), 1.0, 0.0).astype(BF)
        before = dot(present.astype(BF), earlier)
        slot = iota((CAP, TOK), 0).astype(F32)
        wide = jnp.zeros((16, TOK), F32)
        for i in range(8):
            wide = jnp.where(sub16.astype(F32) == rel[i : i + 1], comb[i : i + 1], wide)
        wide = wide.astype(BF)
        for xx in range(NX):
            hit = (slot == before[xx : xx + 1]) & (rows[xx] > 0.5)
            block = jnp.where(hit, 1.0, 0.0).astype(BF)
            sel[c, xx * CAP : (xx + 1) * CAP] = block
            wts[c, xx, :, 0:CAP] = dot(wide, block, ((1,), (1,))).astype(BF)
        xsa[c] = dot(sel[c], ta[c]).astype(BF)
        xin[c, y, rows48(x)] = xsa[c, rows48(x)]
        wtr[c, x, :, 0:CAP] = wts[c, x, :, 0:CAP]

    selection(0)
    pl.semaphore_wait(barrier, len(peers))
    for r in near:
        b_copy(r).start()
    for copy in (za_copy, m_copy):
        for slot, dz in ((1, 1), (2, NZ - 1)):
            copy(0, slot, at_z(z + dz)).start()

    def forward_a(c):
        for copy in (m_copy, za_copy):
            copy(0, c, at_z(z)).wait_recv()
        for copy in (m_copy, za_copy):
            copy(c, c + 2, at_z(z + jnp.where(c % 2 == 1, 1, NZ - 1))).start()

    def forward_b(c):
        @pl.when(c == 0)
        def _():
            for r in near:
                b_arrival(r).wait_recv()
            zb_copy(0, 1, at_z(z + 1)).start()
            zb_copy(0, 2, at_z(z + NZ - 1)).start()

        @pl.when(c > 0)
        def _():
            zb_copy(0, c, at_z(z)).wait_recv()
            zb_copy(c, c + 2, at_z(z + jnp.where(c % 2 == 1, 1, NZ - 1))).start()

    def select_a(c):
        @pl.when(c >= NZ - 2)
        def _():
            for copy in (m_copy, za_copy):
                copy(0, c, at_z(z)).wait_recv()

        @pl.when(c > 0)
        def _():
            selection(c)

        for r in near:
            to_x(xa_copy, c, r).start()
        for r in near:
            to_x(xw_copy, c, r).start()

    def select_b(c):
        @pl.when(c >= NZ - 2)
        def _():
            zb_copy(0, c, at_z(z)).wait_recv()

        xsb[c] = dot(sel[c], tb[c]).astype(BF)
        xrb[c, rows48(x)] = xsb[c, rows48(x)]
        for r in near:
            to_x(xb_copy, c, r).start()

    def gather1(c):
        for r in near:
            from_x(xa_copy, c, r).wait_recv()
        for k in range(2):
            g1_copy(c, k).start()

    def gather2(c):
        for k in range(2):
            g1_arrival(c, k).wait_recv()
            g2_copy(c, k).start()

    def ffn(c):
        for r in near:
            from_x(xw_copy, c, r).wait_recv()
            from_x(xb_copy, c, r).wait_recv()
        for k in range(2):
            g2_arrival(c, k).wait_recv()
        for j in range(NT):
            x_all[:, j * SLICE : j * SLICE + AD] = xin[c, j]
            x_all[:, j * SLICE + AD : (j + 1) * SLICE] = xrb[c, :, BD * j : BD * (j + 1)]
        rows_in = x_all[...]
        for n in range(HID // 256):
            cols = slice(n * 256, (n + 1) * 256)
            gate = dot(rows_in, wg[cols], ((1,), (1,)))
            up = dot(rows_in, wu[cols], ((1,), (1,)))
            scale = jnp.concatenate(
                [dot(wtr[c, xx, :, 0:CAP], expand[:, cols], ((0,), (0,))) for xx in range(NX)], axis=0
            )
            hid[:, cols] = (gate / (1.0 + jnp.exp(-gate)) * up * scale).astype(BF)
        h = hid[...]
        for r in (2, 1, 3, 0):
            j = (y + r) % NT
            for n in range(SLICE // 256):
                lo = n * 256
                part = dot(h, wd[:, pl.ds(pl.multiple_of(j * SLICE + lo, 128), 256)]).astype(BF)
                split = min(max(AR - lo, 0), 256)
                if split:
                    pa[c, j, :, lo : lo + split] = part[:, :split]
                if split < 256:
                    at = pl.multiple_of(BR * j + lo + split - AR, 128)
                    pb[c, :, pl.ds(at, 256 - split)] = part[:, split:]
            if r == 1:
                for k in range(2):
                    s1_copy(c, k).start()

    def scatter1(c):
        for k in range(2):
            to = ym if k else yp
            part = slice(k * HALF, (k + 1) * HALF)
            s1_copy(c, k).wait_recv()
            pa[c, to, part] = (pa[c, to, part].astype(F32) + r1[c, k].astype(F32)).astype(BF)
            s2_copy(c, k).start()

    def scatter2(c):
        for k in range(2):
            s2_copy(c, k).wait_recv()
        qa[c] = (pa[c, y].astype(F32) + r2[c, 0].astype(F32) + r2[c, 1].astype(F32)).astype(BF)
        for r in near:
            to_x(ya_copy, c, r).start()
        xba[c, rows48(x)] = qa[c, rows48(x)]

    def return_b(c):
        for r in near:
            to_x(yb_copy, c, r).start()
        xbb[c, rows48(x)] = pb[c, rows48(x)]

    def unselect_a(c):
        for r in near:
            from_x(ya_copy, c, r).wait_recv()
        sha[c] = dot(sel[c], xba[c], ((0,), (0,)))

    def unselect_b(c):
        for r in near:
            from_x(yb_copy, c, r).wait_recv()
        shb[c] = dot(sel[c], xbb[c], ((0,), (0,)))

    def merge(c, joins, copy, share, out, arrived):
        @pl.when(joins)
        def _():
            copy(c + 2).wait_recv()
            out[c] = (share[c] + arrived[c + 2].astype(F32)).astype(BF)

        @pl.when(jnp.logical_not(joins))
        def _():
            out[c] = share[c].astype(BF)

        copy(c).start()

    def merge_a(c):
        merge(c, (c >= 3) & (c < NZ - 2), ca_copy, sha, zsa, zra)

    def merge_b(c):
        merge(c, c < NZ - 2, cb_copy, shb, zsb, zrb)

    def finish_b(c):
        for k in (1, 2):
            cb_copy(k).wait_recv()
        shb[0] += zrb[1].astype(F32) + zrb[2].astype(F32)
        for r in near:
            bs[r - 1] = shb[0, :, bcol((y + r) % NT, BR)].astype(BF)
            bb_copy(r).start()

    stages = dict(
        forward_a=forward_a, forward_b=forward_b, select_a=select_a, select_b=select_b,
        gather1=gather1, gather2=gather2, ffn=ffn, scatter1=scatter1, scatter2=scatter2,
        return_b=return_b, unselect_a=unselect_a, unselect_b=unselect_b,
        merge_a=merge_a, merge_b=merge_b, finish_b=finish_b,
    )
    first_ffn = min(dict(SCHEDULE)["ffn"])

    def step(i, carry):
        @pl.when(i == first_ffn)
        def _():
            for load in loads:
                load.wait()

        for name, slots in SCHEDULE:
            chunk = jnp.int32(-1)
            for c, slot in enumerate(slots):
                if slot >= 0:
                    chunk = jnp.where(i == slot, c, chunk)

            @pl.when(chunk >= 0)
            def _(name=name, chunk=chunk):
                stages[name](chunk)

        return carry

    lax.fori_loop(0, SLOTS, step, 0)

    total = shb[0, :, bcol(y, BR)]
    for r in near:
        bb_copy(r).wait_recv()
        total = total + br[r - 1].astype(F32)
    outv[:, AR:SLICE] = total.astype(BF)
    total = sha[0]
    for c in (4, 3, 2, 1):
        ca_copy(c).wait_recv()
        total = total + zra[c].astype(F32)
    outv[:, 0:AR] = total.astype(BF)
    result = pltpu.make_async_copy(outv, out_hbm, out_sem)
    result.start()

    def drain(c, carry):
        for k in range(2):
            for cp in (g1_copy, g2_copy, s1_copy, s2_copy):
                cp(c, k).wait_send()
        for r in near:
            for cp in (xa_copy, xw_copy, xb_copy, ya_copy, yb_copy):
                to_x(cp, c, r).wait_send()

        @pl.when(c > 0)
        def _():
            for copy in (m_copy, za_copy, zb_copy):
                copy(0, c, at_z(z)).wait_send()
            ca_copy(c).wait_send()
            cb_copy(c).wait_send()

        return carry

    lax.fori_loop(0, NZ, drain, 0)
    for r in near:
        b_copy(r).wait_send()
        bb_copy(r).wait_send()
    result.wait()


def per_device(tokens, expert_ids, combine_weight, gate_weight, up_weight, down_weight):
    flat = (HID, DM)
    hbm = pl.BlockSpec(memory_space=pl.ANY)
    dma = pltpu.SemaphoreType.DMA

    def vmem(*shape, dtype=BF):
        return pltpu.VMEM(shape, dtype)

    return pl.pallas_call(
        kernel,
        out_shape=jax.ShapeDtypeStruct((TOK, SLICE), BF),
        in_specs=[hbm] * 6,
        out_specs=hbm,
        scratch_shapes=[
            vmem(*flat), vmem(*flat), vmem(*flat),
            vmem(16, HID), vmem(8, TOK, dtype=jnp.int32), vmem(8, TOK),
            vmem(NZ, TOK, AD), vmem(NZ, TOK, NT * BD), vmem(NZ, 16, TOK), vmem(NZ, ROWS, TOK),
            vmem(NZ, ROWS, AD), vmem(NZ, ROWS, NT * BD), vmem(NZ, ROWS, NT * BD),
            vmem(NZ, NX, 16, 128), vmem(NZ, NX, 16, 128),
            vmem(NZ, NT, ROWS, AD), vmem(ROWS, DM), vmem(ROWS, HID),
            vmem(NZ, NT, ROWS, AR), vmem(NZ, ROWS, NT * BR),
            vmem(NZ, 2, HALF, AR), vmem(NZ, 2, ROWS, AR), vmem(NZ, ROWS, AR),
            vmem(NZ, ROWS, AR), vmem(NZ, ROWS, NT * BR),
            vmem(NZ, TOK, AR, dtype=F32), vmem(NZ, TOK, NT * BR, dtype=F32),
            vmem(NZ, TOK, AR), vmem(NZ, TOK, NT * BR),
            vmem(NZ, TOK, AR), vmem(NZ, TOK, NT * BR),
            vmem(NT - 1, TOK, BR), vmem(NT - 1, TOK, BR), vmem(TOK, SLICE),
            dma((3,)), dma((4,)), dma,
            *[dma((NZ,))] * 6,
            *[dma((NZ, 3))] * 6,
            *[dma((NZ, 2))] * 8,
            *[dma((NZ, 3))] * 4,
            *[dma((NZ,))] * 4,
            *[dma((3,))] * 4,
        ],
        compiler_params=pltpu.CompilerParams(
            collective_id=0, has_side_effects=True, vmem_limit_bytes=60 * 2**20
        ),
        name="moe",
    )(
        tokens, expert_ids.T, combine_weight.T,
        gate_weight.reshape(flat), up_weight.reshape(flat), down_weight.reshape(flat),
    )


def solution(mesh):
    in_specs = (
        P(("dp", "expert"), "tensor"),
        P(("dp", "expert"), None),
        P(("dp", "expert"), None),
        P("expert", "tensor", None),
        P("expert", "tensor", None),
        P("expert", "tensor", None),
    )
    out_specs = P(("dp", "expert"), "tensor")
    return jax.shard_map(
        per_device, mesh=mesh, in_specs=in_specs, out_specs=out_specs, check_vma=False
    )
```

```python
import jax
import jax.numpy as jnp
from jax import lax
from jax.experimental import pallas as pl
from jax.experimental.pallas import tpu as pltpu
from jax.sharding import PartitionSpec as P

NT = 4
NX = 4
NZ = 8
TOK = 128
CAP = 48
ROWS = NX * CAP
HALF = ROWS // 2
SLICE = 512
AD = 256
AR = 384
BD = SLICE - AD
BR = SLICE - AR
HID = 768
DM = NT * SLICE
BF = jnp.bfloat16
F32 = jnp.float32

SLOTS = 45
SCHEDULE = (
    ("scatter2", (44, 24, 40, 39, 37, 33, 32, 29)),
    ("merge_a", (-1, 28, 44, 43, 42, 39, 38, 35)),
    ("select_a", (0, 1, 2, 6, 7, 11, 10, 15)),
    ("forward_a", (-1, 0, 1, 4, 6, 9, -1, -1)),
    ("scatter1", (39, 20, 31, 33, 21, 24, 27, 26)),
    ("gather2", (5, 9, 11, 15, 16, 18, 17, 20)),
    ("unselect_b", (44, 41, 35, 36, 33, 25, 29, 27)),
    ("forward_b", (1, 7, 8, 12, 13, 18, -1, -1)),
    ("finish_b", (44, -1, -1, -1, -1, -1, -1, -1)),
    ("select_b", (3, 7, 11, 21, 16, 18, 19, 20)),
    ("gather1", (2, 3, 4, 9, 11, 14, 13, 17)),
    ("merge_b", (-1, 41, 40, 36, 35, 30, 29, 27)),
    ("ffn", (11, 16, 18, 27, 19, 20, 22, 23)),
    ("return_b", (41, 34, 25, 29, 26, 21, 24, 23)),
    ("unselect_a", (44, 27, 43, 42, 41, 38, 37, 33)),
)


def dot(a, b, dims=((1,), (0,))):
    return lax.dot_general(a, b, (dims, ((), ())), preferred_element_type=F32)


def iota(shape, dim):
    return lax.broadcasted_iota(jnp.int32, shape, dim)


def kernel(
    tok_hbm, ids_hbm, comb_hbm, gate_hbm, up_hbm, down_hbm, out_hbm,
    wg, wu, wd, expand, ids_v, comb_v, ta, tb, meta, sel, xsa, xsb, xrb, wts, wtr, xin, x_all, hid,
    pa, pb, r1, r2, qa, xba, xbb, sha, shb, zsa, zsb, zra, zrb, bs, br, outv,
    w_sem, in_sem, out_sem, m_s, m_r, za_s, za_r, zb_s, zb_r, xa_s, xa_r, xw_s, xw_r, xb_s, xb_r,
    g1_s, g1_r, g2_s, g2_r, s1_s, s1_r, s2_s, s2_r, ya_s, ya_r, yb_s, yb_r, ca_s, ca_r, cb_s, cb_r,
    b_s, b_r, bb_s, bb_r,
):
    y = lax.axis_index("tensor")
    e = lax.axis_index("expert")
    z = e // NX
    x = e % NX
    yp = (y + 1) % NT
    yo = (y + 2) % NT
    ym = (y + 3) % NT

    def at_y(j):
        return {"tensor": j}

    def at_x(j):
        return {"expert": z * NX + j}

    def at_z(j):
        return {"expert": (j % NZ) * NX + x}

    def rcopy(src, dst, ssem, rsem, dev):
        return pltpu.make_async_remote_copy(
            src_ref=src, dst_ref=dst, send_sem=ssem, recv_sem=rsem,
            device_id=dev, device_id_type=pl.DeviceIdType.MESH,
        )

    def rows48(j):
        return pl.ds(pl.multiple_of(j * CAP, 16), CAP)

    def bcol(j, width):
        return pl.ds(pl.multiple_of(width * j, 128), width)

    def m_copy(src, slot, dev):
        return rcopy(meta.at[src], meta.at[slot], m_s.at[slot], m_r.at[slot], dev)

    def za_copy(src, slot, dev):
        return rcopy(ta.at[src], ta.at[slot], za_s.at[slot], za_r.at[slot], dev)

    def zb_copy(src, slot, dev):
        return rcopy(tb.at[src], tb.at[slot], zb_s.at[slot], zb_r.at[slot], dev)

    def xa_copy(c, r, frm, to):
        return rcopy(
            xsa.at[c, rows48(to)], xin.at[c, y, rows48(frm)],
            xa_s.at[c, r - 1], xa_r.at[c, r - 1], at_x(to),
        )

    def xw_copy(c, r, frm, to):
        return rcopy(wts.at[c, to], wtr.at[c, frm], xw_s.at[c, r - 1], xw_r.at[c, r - 1], at_x(to))

    def xb_copy(c, r, frm, to):
        return rcopy(
            xsb.at[c, rows48(to)], xrb.at[c, rows48(frm)],
            xb_s.at[c, r - 1], xb_r.at[c, r - 1], at_x(to),
        )

    def ya_copy(c, r, frm, to):
        return rcopy(
            qa.at[c, rows48(to)], xba.at[c, rows48(frm)],
            ya_s.at[c, r - 1], ya_r.at[c, r - 1], at_x(to),
        )

    def yb_copy(c, r, frm, to):
        return rcopy(
            pb.at[c, rows48(to)], xbb.at[c, rows48(frm)],
            yb_s.at[c, r - 1], yb_r.at[c, r - 1], at_x(to),
        )

    def to_x(copy, c, r):
        return copy(c, r, x, (x + r) % NX)

    def from_x(copy, c, r):
        frm = (x + NX - r) % NX
        return copy(c, r, frm, frm)

    def g1_copy(c, k):
        return rcopy(xin.at[c, y], xin.at[c, y], g1_s.at[c, k], g1_r.at[c, k], at_y(ym if k else yp))

    def g1_arrival(c, k):
        frm = yp if k else ym
        return rcopy(xin.at[c, frm], xin.at[c, frm], g1_s.at[c, k], g1_r.at[c, k], at_y(frm))

    def g2_copy(c, k):
        blk = xin.at[c, yp if k else ym, pl.ds(k * HALF, HALF)]
        return rcopy(blk, blk, g2_s.at[c, k], g2_r.at[c, k], at_y(ym if k else yp))

    def g2_arrival(c, k):
        blk = xin.at[c, yo, pl.ds(k * HALF, HALF)]
        return rcopy(blk, blk, g2_s.at[c, k], g2_r.at[c, k], at_y(yp if k else ym))

    def s1_copy(c, k):
        return rcopy(
            pa.at[c, yo, pl.ds(k * HALF, HALF)], r1.at[c, k],
            s1_s.at[c, k], s1_r.at[c, k], at_y(ym if k else yp),
        )

    def s2_copy(c, k):
        to = ym if k else yp
        return rcopy(pa.at[c, to], r2.at[c, k], s2_s.at[c, k], s2_r.at[c, k], at_y(to))

    def homeward(c, hops):
        return at_z(jnp.where(c % 2 == 1, z + NZ - hops, z + hops))

    def ca_copy(c):
        hops = jnp.where((c + 1) // 2 == 2, 2, 1)
        return rcopy(zsa.at[c], zra.at[c], ca_s.at[c], ca_r.at[c], homeward(c, hops))

    def cb_copy(c):
        return rcopy(zsb.at[c], zrb.at[c], cb_s.at[c], cb_r.at[c], homeward(c, 1))

    def b_copy(r):
        blk = tb.at[0, :, bcol(y, BD)]
        return rcopy(blk, blk, b_s.at[r - 1], b_r.at[r - 1], at_y((y + r) % NT))

    def b_arrival(r):
        frm = (y + NT - r) % NT
        blk = tb.at[0, :, bcol(frm, BD)]
        return rcopy(blk, blk, b_s.at[r - 1], b_r.at[r - 1], at_y(frm))

    def bb_copy(r):
        return rcopy(bs.at[r - 1], br.at[r - 1], bb_s.at[r - 1], bb_r.at[r - 1], at_y((y + r) % NT))

    near = (2, 1, 3)

    inputs = [
        pltpu.make_async_copy(src, dst, in_sem.at[k])
        for k, (src, dst) in enumerate((
            (tok_hbm.at[:, pl.ds(AD, BD)], tb.at[0, :, bcol(y, BD)]),
            (ids_hbm, ids_v),
            (comb_hbm, comb_v),
            (tok_hbm.at[:, pl.ds(0, AD)], ta.at[0]),
        ))
    ]
    loads = [
        pltpu.make_async_copy(src, dst, w_sem.at[k])
        for k, (src, dst) in enumerate(((gate_hbm, wg), (up_hbm, wu), (down_hbm, wd)))
    ]
    for load in inputs:
        load.start()

    barrier = pltpu.get_barrier_semaphore()
    peers = [at_y((y + r) % NT) for r in range(1, NT)]
    peers += [at_x((x + r) % NX) for r in range(1, NX)]
    peers += [at_z(z + r) for r in (1, NZ - 1, 2, NZ - 2)]
    for peer in peers:
        pl.semaphore_signal(barrier, 1, device_id=peer, device_id_type=pl.DeviceIdType.MESH)
    for load in loads:
        load.start()

    base = (iota((16, HID), 0) - NX * x) * (HID // NX)
    hid_n = iota((16, HID), 1)
    expand[...] = jnp.where((hid_n >= base) & (hid_n < base + HID // NX), 1.0, 0.0).astype(BF)
    for load in inputs:
        load.wait()
    meta[0] = jnp.concatenate([ids_v[...].astype(F32), comb_v[...].astype(F32)], axis=0).astype(BF)

    def selection(c):
        info = meta[c].astype(F32)
        rel = info[0:8] - jnp.asarray(NX * NX * z, F32)
        comb = info[8:16]
        sub16 = iota((16, TOK), 0)
        present = jnp.zeros((16, TOK), F32)
        rows = []
        for xx in range(NX):
            inside = (rel >= float(NX * xx)) & (rel < float(NX * xx + NX))
            row = jnp.max(jnp.where(inside, 1.0, 0.0), axis=0, keepdims=True)
            rows.append(row)
            present = jnp.where(sub16 == xx, row, present)
        earlier = jnp.where(iota((TOK, TOK), 0) < iota((TOK, TOK), 1), 1.0, 0.0).astype(BF)
        before = dot(present.astype(BF), earlier)
        slot = iota((CAP, TOK), 0).astype(F32)
        wide = jnp.zeros((16, TOK), F32)
        for i in range(8):
            wide = jnp.where(sub16.astype(F32) == rel[i : i + 1], comb[i : i + 1], wide)
        wide = wide.astype(BF)
        for xx in range(NX):
            hit = (slot == before[xx : xx + 1]) & (rows[xx] > 0.5)
            block = jnp.where(hit, 1.0, 0.0).astype(BF)
            sel[c, xx * CAP : (xx + 1) * CAP] = block
            wts[c, xx, :, 0:CAP] = dot(wide, block, ((1,), (1,))).astype(BF)
        xsa[c] = dot(sel[c], ta[c]).astype(BF)
        xin[c, y, rows48(x)] = xsa[c, rows48(x)]
        wtr[c, x, :, 0:CAP] = wts[c, x, :, 0:CAP]

    selection(0)
    pl.semaphore_wait(barrier, len(peers))
    for r in near:
        b_copy(r).start()
    for copy in (za_copy, m_copy):
        for slot, dz in ((1, 1), (2, NZ - 1)):
            copy(0, slot, at_z(z + dz)).start()

    def forward_a(c):
        for copy in (m_copy, za_copy):
            copy(0, c, at_z(z)).wait_recv()
        for copy in (m_copy, za_copy):
            copy(c, c + 2, at_z(z + jnp.where(c % 2 == 1, 1, NZ - 1))).start()

    def forward_b(c):
        @pl.when(c == 0)
        def _():
            for r in near:
                b_arrival(r).wait_recv()
            zb_copy(0, 1, at_z(z + 1)).start()
            zb_copy(0, 2, at_z(z + NZ - 1)).start()

        @pl.when(c > 0)
        def _():
            zb_copy(0, c, at_z(z)).wait_recv()
            zb_copy(c, c + 2, at_z(z + jnp.where(c % 2 == 1, 1, NZ - 1))).start()

    def select_a(c):
        @pl.when(c >= NZ - 2)
        def _():
            for copy in (m_copy, za_copy):
                copy(0, c, at_z(z)).wait_recv()

        @pl.when(c > 0)
        def _():
            selection(c)

        for r in near:
            to_x(xa_copy, c, r).start()
        for r in near:
            to_x(xw_copy, c, r).start()

    def select_b(c):
        @pl.when(c >= NZ - 2)
        def _():
            zb_copy(0, c, at_z(z)).wait_recv()

        xsb[c] = dot(sel[c], tb[c]).astype(BF)
        xrb[c, rows48(x)] = xsb[c, rows48(x)]
        for r in near:
            to_x(xb_copy, c, r).start()

    def gather1(c):
        for r in near:
            from_x(xa_copy, c, r).wait_recv()
        for k in range(2):
            g1_copy(c, k).start()

    def gather2(c):
        for k in range(2):
            g1_arrival(c, k).wait_recv()
            g2_copy(c, k).start()

    def ffn(c):
        for r in near:
            from_x(xw_copy, c, r).wait_recv()
            from_x(xb_copy, c, r).wait_recv()
        for k in range(2):
            g2_arrival(c, k).wait_recv()
        for j in range(NT):
            x_all[:, j * SLICE : j * SLICE + AD] = xin[c, j]
            x_all[:, j * SLICE + AD : (j + 1) * SLICE] = xrb[c, :, BD * j : BD * (j + 1)]
        rows_in = x_all[...]
        for n in range(HID // 256):
            cols = slice(n * 256, (n + 1) * 256)
            gate = dot(rows_in, wg[cols], ((1,), (1,)))
            up = dot(rows_in, wu[cols], ((1,), (1,)))
            scale = jnp.concatenate(
                [dot(wtr[c, xx, :, 0:CAP], expand[:, cols], ((0,), (0,))) for xx in range(NX)], axis=0
            )
            hid[:, cols] = (gate / (1.0 + jnp.exp(-gate)) * up * scale).astype(BF)
        h = hid[...]
        for r in (2, 1, 3, 0):
            j = (y + r) % NT
            for n in range(SLICE // 256):
                lo = n * 256
                part = dot(h, wd[:, pl.ds(pl.multiple_of(j * SLICE + lo, 128), 256)]).astype(BF)
                split = min(max(AR - lo, 0), 256)
                if split:
                    pa[c, j, :, lo : lo + split] = part[:, :split]
                if split < 256:
                    at = pl.multiple_of(BR * j + lo + split - AR, 128)
                    pb[c, :, pl.ds(at, 256 - split)] = part[:, split:]
            if r == 2:
                for k in range(2):
                    s1_copy(c, k).start()

    def scatter1(c):
        for k in range(2):
            to = ym if k else yp
            part = slice(k * HALF, (k + 1) * HALF)
            s1_copy(c, k).wait_recv()
            pa[c, to, part] = (pa[c, to, part].astype(F32) + r1[c, k].astype(F32)).astype(BF)
            s2_copy(c, k).start()

    def scatter2(c):
        for k in range(2):
            s2_copy(c, k).wait_recv()
        qa[c] = (pa[c, y].astype(F32) + r2[c, 0].astype(F32) + r2[c, 1].astype(F32)).astype(BF)
        for r in near:
            to_x(ya_copy, c, r).start()
        xba[c, rows48(x)] = qa[c, rows48(x)]

    def return_b(c):
        for r in near:
            to_x(yb_copy, c, r).start()
        xbb[c, rows48(x)] = pb[c, rows48(x)]

    def unselect_a(c):
        for r in near:
            from_x(ya_copy, c, r).wait_recv()
        sha[c] = dot(sel[c], xba[c], ((0,), (0,)))

    def unselect_b(c):
        for r in near:
            from_x(yb_copy, c, r).wait_recv()
        shb[c] = dot(sel[c], xbb[c], ((0,), (0,)))

    def merge(c, joins, copy, share, out, arrived):
        @pl.when(joins)
        def _():
            copy(c + 2).wait_recv()
            out[c] = (share[c] + arrived[c + 2].astype(F32)).astype(BF)

        @pl.when(jnp.logical_not(joins))
        def _():
            out[c] = share[c].astype(BF)

        copy(c).start()

    def merge_a(c):
        merge(c, (c >= 3) & (c < NZ - 2), ca_copy, sha, zsa, zra)

    def merge_b(c):
        merge(c, c < NZ - 2, cb_copy, shb, zsb, zrb)

    def finish_b(c):
        for k in (1, 2):
            cb_copy(k).wait_recv()
        shb[0] += zrb[1].astype(F32) + zrb[2].astype(F32)
        for r in near:
            bs[r - 1] = shb[0, :, bcol((y + r) % NT, BR)].astype(BF)
            bb_copy(r).start()

    stages = dict(
        forward_a=forward_a, forward_b=forward_b, select_a=select_a, select_b=select_b,
        gather1=gather1, gather2=gather2, ffn=ffn, scatter1=scatter1, scatter2=scatter2,
        return_b=return_b, unselect_a=unselect_a, unselect_b=unselect_b,
        merge_a=merge_a, merge_b=merge_b, finish_b=finish_b,
    )
    first_ffn = min(dict(SCHEDULE)["ffn"])

    def step(i, carry):
        @pl.when(i == first_ffn)
        def _():
            for load in loads:
                load.wait()

        for name, slots in SCHEDULE:
            chunk = jnp.int32(-1)
            for c, slot in enumerate(slots):
                if slot >= 0:
                    chunk = jnp.where(i == slot, c, chunk)

            @pl.when(chunk >= 0)
            def _(name=name, chunk=chunk):
                stages[name](chunk)

        return carry

    lax.fori_loop(0, SLOTS, step, 0)

    total = shb[0, :, bcol(y, BR)]
    for r in near:
        bb_copy(r).wait_recv()
        total = total + br[r - 1].astype(F32)
    outv[:, AR:SLICE] = total.astype(BF)
    total = sha[0]
    for c in (4, 3, 2, 1):
        ca_copy(c).wait_recv()
        total = total + zra[c].astype(F32)
    outv[:, 0:AR] = total.astype(BF)
    result = pltpu.make_async_copy(outv, out_hbm, out_sem)
    result.start()

    def drain(c, carry):
        for k in range(2):
            for cp in (g1_copy, g2_copy, s1_copy, s2_copy):
                cp(c, k).wait_send()
        for r in near:
            for cp in (xa_copy, xw_copy, xb_copy, ya_copy, yb_copy):
                to_x(cp, c, r).wait_send()

        @pl.when(c > 0)
        def _():
            for copy in (m_copy, za_copy, zb_copy):
                copy(0, c, at_z(z)).wait_send()
            ca_copy(c).wait_send()
            cb_copy(c).wait_send()

        return carry

    lax.fori_loop(0, NZ, drain, 0)
    for r in near:
        b_copy(r).wait_send()
        bb_copy(r).wait_send()
    result.wait()


def per_device(tokens, expert_ids, combine_weight, gate_weight, up_weight, down_weight):
    flat = (HID, DM)
    hbm = pl.BlockSpec(memory_space=pl.ANY)
    dma = pltpu.SemaphoreType.DMA

    def vmem(*shape, dtype=BF):
        return pltpu.VMEM(shape, dtype)

    return pl.pallas_call(
        kernel,
        out_shape=jax.ShapeDtypeStruct((TOK, SLICE), BF),
        in_specs=[hbm] * 6,
        out_specs=hbm,
        scratch_shapes=[
            vmem(*flat), vmem(*flat), vmem(*flat),
            vmem(16, HID), vmem(8, TOK, dtype=jnp.int32), vmem(8, TOK),
            vmem(NZ, TOK, AD), vmem(NZ, TOK, NT * BD), vmem(NZ, 16, TOK), vmem(NZ, ROWS, TOK),
            vmem(NZ, ROWS, AD), vmem(NZ, ROWS, NT * BD), vmem(NZ, ROWS, NT * BD),
            vmem(NZ, NX, 16, 128), vmem(NZ, NX, 16, 128),
            vmem(NZ, NT, ROWS, AD), vmem(ROWS, DM), vmem(ROWS, HID),
            vmem(NZ, NT, ROWS, AR), vmem(NZ, ROWS, NT * BR),
            vmem(NZ, 2, HALF, AR), vmem(NZ, 2, ROWS, AR), vmem(NZ, ROWS, AR),
            vmem(NZ, ROWS, AR), vmem(NZ, ROWS, NT * BR),
            vmem(NZ, TOK, AR, dtype=F32), vmem(NZ, TOK, NT * BR, dtype=F32),
            vmem(NZ, TOK, AR), vmem(NZ, TOK, NT * BR),
            vmem(NZ, TOK, AR), vmem(NZ, TOK, NT * BR),
            vmem(NT - 1, TOK, BR), vmem(NT - 1, TOK, BR), vmem(TOK, SLICE),
            dma((3,)), dma((4,)), dma,
            *[dma((NZ,))] * 6,
            *[dma((NZ, 3))] * 6,
            *[dma((NZ, 2))] * 8,
            *[dma((NZ, 3))] * 4,
            *[dma((NZ,))] * 4,
            *[dma((3,))] * 4,
        ],
        compiler_params=pltpu.CompilerParams(
            collective_id=0, has_side_effects=True, vmem_limit_bytes=60 * 2**20
        ),
        name="moe",
    )(
        tokens, expert_ids.T, combine_weight.T,
        gate_weight.reshape(flat), up_weight.reshape(flat), down_weight.reshape(flat),
    )


def solution(mesh):
    in_specs = (
        P(("dp", "expert"), "tensor"),
        P(("dp", "expert"), None),
        P(("dp", "expert"), None),
        P("expert", "tensor", None),
        P("expert", "tensor", None),
        P("expert", "tensor", None),
    )
    out_specs = P(("dp", "expert"), "tensor")
    return jax.shard_map(
        per_device, mesh=mesh, in_specs=in_specs, out_specs=out_specs, check_vma=False
    )
```
